256 devices in a mesh: seq: 16 (over y_hi, z), head: 16 (over y_lo, x, core).
Axes of the slice: x: 4, y: 4 (y_hi: 2, y_lo: 2; y = y_hi * 2 + y_lo), z: 8, core: 2. Of those that a mesh axis runs over, the one named last changes fastest.
Arguments:
- queries: bfloat16 [16384, 4096], P(('seq', 'head')), may hold values from -9 to 9, as said below
- keys: bfloat16 [16384, 512], P(('seq', 'head')), may hold values from -9 to 9, as said below
- values: bfloat16 [16384, 512], P(('seq', 'head')), may hold values from -6 to 6
Outputs:
- attended: bfloat16 [16384, 4096], P(('seq', 'head'))
The draws below stay inside these ranges and needn't reach their ends.
Inputs may be any that keep to these rules, and one draw needn't show every extreme that they name: `queries`: query entries are of order one except on a few rows. `keys`: key entries are of order one except on a few rows.
All inputs are finite; a program needn't handle non-finite values.
Results may differ from the reference program's by a relative error of at most 0.005.
Values may be sent and summed in bfloat16 or wider, within the bound.
A program may use at most 64 MiB of HBM per device.

```python
import math
import jax
import jax.numpy as jnp
from jax import lax

H = 32
KV = 4
DH = 128
TOKENS = 16384


def paired(key):
    base = jax.random.fold_in(key, 7)
    key_q, key_k = jax.random.split(base, 2)
    query_mat = jnp.clip(jax.random.normal(key_q, (TOKENS, H * DH), jnp.float32), -6.0, 6.0)
    key_mat = jnp.clip(jax.random.normal(key_k, (TOKENS, KV * DH), jnp.float32), -6.0, 6.0)
    return (query_mat, key_mat)


def draw_queries(key, part):
    return paired(key)[0].astype(jnp.bfloat16)


def draw_keys(key, part):
    return paired(key)[1].astype(jnp.bfloat16)


def shard_levels(key, dims, pieces, smallest, high):
    factor_of, own = 1.0, jax.random.fold_in(key, 6)
    for position, shards_of in pieces:
        draws = jnp.exp(jax.random.uniform(jax.random.fold_in(own, position), (shards_of,), jnp.float32, smallest / len(pieces), high / len(pieces)))
        factor_of = factor_of * jnp.repeat(draws, dims[position] // shards_of).reshape([-1 if axis == position else 1 for axis in range(len(dims))])
    return factor_of


def scatter_about(rng, dims, spread, bound, shards=(), kind=jnp.bfloat16):
    array = spread * jax.random.normal(rng, dims, jnp.float32)
    if shards:
        array = array * shard_levels(rng, dims, shards, -0.22, 0.18)
    return jnp.clip(array, -bound, bound).astype(kind)


def setup_inputs(seed: int = 0) -> dict:
    seeds = jax.random.split(jax.random.key(seed), 4)
    queries = draw_queries(jax.random.fold_in(seeds[3], 71), 0)
    keys = draw_keys(jax.random.fold_in(seeds[3], 71), 0)
    values = scatter_about(seeds[2], (TOKENS, KV * DH), 1.0, 6.0, ((0, 256),))
    return dict(queries=queries, keys=keys, values=values)


def reference(queries, keys, values):
    length = queries.shape[0]
    block = min(1024, length)
    blocks = length // block
    group = H // KV
    scale = 1.0 / math.sqrt(DH)
    q_heads = queries.reshape(length, H, DH)
    k_heads = keys.reshape(length, KV, DH)
    v_heads = values.reshape(length, KV, DH)
    key_pos = jnp.arange(length, dtype=jnp.int32)

    def one_head(head):
        q_mat = lax.dynamic_index_in_dim(q_heads, head, 1, keepdims=False)
        k_mat = lax.dynamic_index_in_dim(k_heads, head // group, 1, keepdims=False)
        v_mat = lax.dynamic_index_in_dim(v_heads, head // group, 1, keepdims=False)

        def one_block(index):
            first = (index * block).astype(jnp.int32)
            rows = lax.dynamic_slice_in_dim(q_mat, first, block, 0)
            scores = jnp.dot(rows, k_mat.T, preferred_element_type=jnp.float32) * scale
            query_pos = first + jnp.arange(block, dtype=jnp.int32)
            scores = jnp.where(key_pos[None, :] <= query_pos[:, None], scores, -jnp.inf)
            rowmax = lax.optimization_barrier(jnp.max(scores, axis=1, keepdims=True))
            expo = jnp.exp(scores - rowmax)
            total = lax.optimization_barrier(jnp.sum(expo, axis=1, keepdims=True))
            numer = jnp.dot(expo.astype(jnp.bfloat16), v_mat, preferred_element_type=jnp.float32)
            return (numer / total).astype(jnp.bfloat16)
        return lax.map(one_block, jnp.arange(blocks, dtype=jnp.int32)).reshape(length, DH)
    result = lax.map(one_head, jnp.arange(H, dtype=jnp.int32))
    return result.transpose(1, 0, 2).reshape(length, H * DH)
```

```python
import functools
import math

import jax
import jax.numpy as jnp
from jax import lax
from jax.experimental import pallas as pl
from jax.experimental.pallas import tpu as pltpu
from jax.sharding import PartitionSpec as P

H = 32
KV = 4
DH = 128
GROUP = H // KV
NX, NY, NZ = 4, 4, 8
TILES = 8
SLAB = 1024
CHUNK = 256
SCALE = math.log2(math.e) / math.sqrt(DH)
ZI_OF = (0, 2, 1, 3)
f32 = jnp.float32
bf16 = jnp.bfloat16


def rem(a, b):
    return lax.rem(a, jnp.int32(b))


def div(a, b):
    return lax.div(a, jnp.int32(b))


def tie(z):
    return rem(z + 6 + 4 * rem(div(z, 2), 2), NZ)


def zsrc(z, zi):
    far = rem(z + 6 + 4 * rem(div(z, 2), 2), NZ)
    near = jnp.where(zi == 0, z, jnp.where(zi == 1, rem(z + 1, NZ), rem(z + 7, NZ)))
    return jnp.where(zi == 3, far, near)


def device(x, y, z, c):
    return (div(y, 2) * NZ + z, rem(y, 2) * 8 + x * 2 + c)


def kernel(
    q_hbm, k_hbm, v_hbm, o_ref, kv, q_own, k_own, v_own, q_in, qt, o_stage, mx, tot, acc, s_buf,
    lsem, zsend, zrecv, qsend, qrecv, gsend, grecv, csend, crecv, osend, orecv,
):
    seq = lax.axis_index("seq")
    head = lax.axis_index("head")
    yhi = div(seq, NZ)
    z = rem(seq, NZ)
    ylo = div(head, 8)
    x = rem(div(head, 2), 4)
    c = rem(head, 2)
    y = yhi * 2 + ylo
    oc = 1 - c
    oy = 3 - y
    blk = ylo * 4 + x
    kind = rem(z, KV)

    def remote(src, dst, ssem, rsem, where):
        return pltpu.make_async_remote_copy(
            src_ref=src, dst_ref=dst, send_sem=ssem, recv_sem=rsem,
            device_id=where, device_id_type=pl.DeviceIdType.MESH,
        )

    def local(src, dst, sem):
        return pltpu.make_async_copy(src, dst, sem)

    loads = [
        local(k_hbm, k_own, lsem.at[0]), local(v_hbm, v_own, lsem.at[1]), local(q_hbm, q_own, lsem.at[2]),
    ]
    for load in loads:
        load.start()

    def kv_cols(zz):
        return pl.ds(pl.multiple_of(rem(zz, KV) * DH, DH), DH)

    kept = [
        local(k_hbm.at[:, kv_cols(z)], kv.at[0, yhi, z, blk, c], lsem.at[3]),
        local(v_hbm.at[:, kv_cols(z)], kv.at[1, yhi, z, blk, c], lsem.at[4]),
    ]
    for load in kept:
        load.start()

    tz = [z, rem(z + 1, NZ), rem(z + 7, NZ), tie(z)]
    cs = (c, oc)
    ys = (y, oy)

    barrier = pltpu.get_barrier_semaphore()

    def greet(where):
        pl.semaphore_signal(barrier, inc=1, device_id=where, device_id_type=pl.DeviceIdType.MESH)

    greeted = 0
    for j in range(4):
        for yy in range(2):
            for k in range(2):
                if j or yy or k:
                    greet(device(x, ys[yy], tz[j], cs[k]))
                    greeted += 1
    for zz in (rem(z + 3, NZ), rem(z + 4, NZ), rem(z + 5, NZ), rem(2 * z + NZ - tz[3], NZ)):
        greet(device(x, y, zz, c))
        greeted += 1
    for where in (
        device(rem(x + 1, NX), y, z, c), device(rem(x + 3, NX), y, z, c), device(x, yhi * 2 + 1 - ylo, z, c),
    ):
        greet(where)
        greeted += 1

    for load in loads:
        load.wait()
    pl.semaphore_wait(barrier, greeted)

    own = (k_own, v_own)

    def z_copy(dz, n):
        zz = rem(z + dz, NZ)
        return remote(
            own[n].at[:, kv_cols(zz)], kv.at[n, yhi, z, blk, c], zsend.at[n, dz], zrecv.at[n, dz], device(x, y, zz, c)
        )

    def z_landed(dz, n):
        zz = rem(z + NZ - dz, NZ)
        remote(
            own[n].at[:, kv_cols(z)], kv.at[n, yhi, zz, blk, c], zsend.at[n, dz], zrecv.at[n, dz], device(x, y, zz, c)
        ).wait_recv()

    z_order = (4, 3, 5, 2, 6, 1, 7)
    for dz in z_order:
        for n in range(2):
            z_copy(dz, n).start()
    for load in kept:
        load.wait()

    def q_cols(j, yy, k):
        yh = div(ys[yy], 2)
        first = rem(tz[j], KV) * GROUP + 4 * yh + 2 * cs[k]
        return pl.ds(pl.multiple_of(first * DH, 2 * DH), 2 * DH)

    def q_copy(j, yy, k):
        tile = yy * 4 + ZI_OF[j]
        return remote(
            q_own.at[:, q_cols(j, yy, k)], q_in.at[tile, c], qsend.at[(j * 2 + yy) * 2 + k], qrecv.at[tile, c],
            device(x, ys[yy], tz[j], cs[k]),
        )

    def q_landed(tile, k):
        yy, zi = divmod(tile, 4)
        zz = (z, tz[1], tz[2], tz[3])[zi]
        remote(
            q_own.at[:, pl.ds(0, 2 * DH)], q_in.at[tile, cs[k]], qsend.at[0], qrecv.at[tile, cs[k]],
            device(x, ys[yy], zz, cs[k]),
        ).wait_recv()

    for yy in (1, 0):
        for j in (3, 1, 2, 0):
            for k in range(2):
                if j or yy or k:
                    q_copy(j, yy, k).start()
    q_in[0, c] = q_own[:, q_cols(0, 0, 0)]

    for dz in z_order:
        for n in range(2):
            z_landed(dz, n)

    def a_dev(d):
        return device(rem(x + d * (1 - c), NX), rem(y + d * c, NY), z, c)

    def b_dev(d):
        return device(rem(x + d * c, NX), rem(y + d * (1 - c), NY), z, c)

    def block(ra, rb):
        xk = rem(x + ra * (1 - c) + rb * c, NX)
        yk = rem(y + ra * c + rb * (1 - c), NY)
        return div(yk, 2), rem(yk, 2) * 4 + xk

    def piece(ra, rb, n, core):
        yh, q = block(ra, rb)
        if n is None:
            return kv.at[:, yh, :, q, core]
        return kv.at[n, yh, :, q, core]

    def g_copy(index, ra, rb, n, axis, d):
        ref = piece(ra, rb, n, c)
        to = a_dev(d % 4) if axis == 0 else b_dev(d % 4)
        if axis == 0:
            there = ((ra - d) % 4, rb)
        else:
            there = (ra, (rb - d) % 4)
        return remote(ref, ref, gsend.at[index], grecv.at[there[0], there[1], n or 0], to)

    def g_landed(ra, rb, n):
        ref = piece(ra, rb, n, c)
        remote(ref, ref, gsend.at[0], grecv.at[ra, rb, n or 0], a_dev(1)).wait_recv()

    def c_copy(ra, rb):
        yh, q = block(ra, rb)
        ref = piece(ra, rb, None, c)
        return remote(ref, ref, csend.at[yh, q], crecv.at[yh, q], device(x, y, z, oc))

    sends = []

    def send(copy):
        copy.start()
        sends.append(copy)

    def g_send(*what):
        send(g_copy(len(g_list), *what))
        g_list.append(what)

    g_list = []

    def spread(ra, rb, axis):
        for d in (1, -1):
            g_send(ra, rb, None, axis, d)

    spread(0, 0, 0)
    spread(0, 0, 1)
    send(c_copy(0, 0))

    def line(ra, rb, axis, then):
        for d, n in ((1, 0), (-1, 1)):
            here = ((ra - d) % 4, rb) if axis == 0 else (ra, (rb - d) % 4)
            g_landed(*here, None)
            g_send(*here, n, axis, d)
            if then:
                spread(*here, 1)
            send(c_copy(*here))
        far = ((ra + 2) % 4, rb) if axis == 0 else (ra, (rb + 2) % 4)
        return far

    def far_landed(far, then):
        g_landed(*far, 0)
        g_landed(*far, 1)
        if then:
            spread(*far, 1)
        send(c_copy(*far))

    far_a = line(0, 0, 0, True)
    far_b = line(0, 0, 1, False)
    far_landed(far_a, True)
    far_landed(far_b, False)
    for ra in (3, 1, 2):
        far_landed(line(ra, 0, 1, False), False)

    for yh in range(2):
        for q in range(8):
            ref = kv.at[:, yh, :, q, oc]
            remote(ref, ref, csend.at[yh, q], crecv.at[yh, q], device(x, y, z, oc)).wait_recv()

    for tile in range(TILES):
        for k in range(2):
            if tile or k:
                q_landed(tile, k)
        for h in range(2):
            part = q_in[tile, :, :, h * DH : (h + 1) * DH].reshape(2 * 64, DH)
            qt[tile, :, h * DH : (h + 1) * DH] = part.T
    mx[...] = jnp.full(mx.shape, -jnp.inf, f32)
    tot[...] = jnp.zeros(tot.shape, f32)
    acc[...] = jnp.zeros(acc.shape, f32)

    def last_slab(t):
        side = jnp.where(t < 4, yhi, 1 - yhi)
        return side * NZ + zsrc(z, rem(t, 4))

    def segment(n, s, g):
        yh = div(s, NZ)
        zz = rem(s, NZ)
        return jnp.concatenate([kv[n, yh, zz, 2 * g + i].reshape(2 * 64, DH) for i in range(2)], axis=0)

    def fold(v, op):
        return op(v.reshape(v.shape[0] // 8, 8, v.shape[1]), axis=0)

    def score(t, s, g, slot, masked):
        sc = lax.dot_general(
            segment(0, s, g), qt[t], (((1,), (0,)), ((), ())), preferred_element_type=f32
        )
        if masked:
            yl = jnp.where(t < 4, ylo, 1 - ylo)
            row = rem(lax.broadcasted_iota(jnp.int32, sc.shape, 1), 128) + (yl * 4 + x) * 128
            key = lax.broadcasted_iota(jnp.int32, sc.shape, 0) + g * CHUNK
            sc = jnp.where(key <= row, sc, -jnp.inf)
        s_buf[slot, g * CHUNK : (g + 1) * CHUNK] = sc
        return fold(sc, jnp.max)

    def apply(s, g, slot, top8, l8, pv):
        sc = s_buf[slot, g * CHUNK : (g + 1) * CHUNK].reshape(CHUNK // 8, 8, 2 * DH)
        p = jnp.exp2((sc - top8[None]) * SCALE)
        l8 = l8 + jnp.sum(p, axis=0)
        d = lax.dot_general(
            segment(1, s, g), p.reshape(CHUNK, 2 * DH).astype(bf16), (((0,), (0,)), ((), ())),
            preferred_element_type=f32,
        )
        return l8, (d if pv is None else pv + d)

    parts = SLAB // CHUNK

    def o_cols(t):
        return pl.ds(pl.multiple_of((kind * GROUP + 4 * yhi + 2 * c) * DH, 2 * DH), 2 * DH)

    def o_copy(t, k):
        cc = k
        yy = jnp.where(t < 4, y, oy)
        zz = zsrc(z, rem(t, 4))
        return remote(
            o_stage.at[t, cc], o_ref.at[:, o_cols(t)], osend.at[t, cc],
            orecv.at[t, c], device(x, yy, zz, cc),
        )

    def finish(t):
        for h in range(2):
            cols = slice(h * DH, (h + 1) * DH)
            whole = jnp.sum(tot[t, :, cols], axis=0, keepdims=True)
            rows = (acc[t, :, cols] / whole).T.astype(bf16)
            o_stage[t, :, :, cols] = rows.reshape(2, 64, DH)

        for k in range(2):
            @pl.when((t != 0) | (c != k))
            def _():
                o_copy(t, k).start()

    def prep(t, m8):
        old = mx[t]
        top = jnp.maximum(old, jnp.max(m8, axis=0, keepdims=True))
        factor = jnp.exp2((old - top) * SCALE)
        mx[t] = top
        return jnp.broadcast_to(top, (8, 2 * DH)), factor

    def item(t, s, tn, sn, m8, u, masked):
        top8, factor = prep(t, m8)
        l8, pv, nm = tot[t] * factor, None, None
        for g in range(parts):
            r = score(tn, sn, g, 1 - u, masked)
            nm = r if nm is None else jnp.maximum(nm, r)
            l8, pv = apply(s, g, u, top8, l8, pv)
        acc[t] = acc[t] * factor + pv
        tot[t] = l8
        return nm

    count = 0
    for t in range(TILES):
        count = count + last_slab(jnp.int32(t)) + 1

    def first(t, s, masked):
        m8 = None
        for g in range(parts):
            r = score(t, s, g, 0, masked)
            m8 = r if m8 is None else jnp.maximum(m8, r)
        return m8

    zero = jnp.int32(0)
    m8 = lax.cond(last_slab(zero) == 0, lambda: first(zero, zero, True), lambda: first(zero, zero, False))

    def pair(i, carry):
        t, s, m8 = carry
        for u in range(2):
            done = s == last_slab(t)
            tn = jnp.where(done, lax.min(t + 1, TILES - 1), t)
            sn = jnp.where(done, 0, s + 1)
            m8 = lax.cond(
                sn == last_slab(tn),
                lambda m8=m8, u=u, t=t, s=s, tn=tn, sn=sn: item(t, s, tn, sn, m8, u, True),
                lambda m8=m8, u=u, t=t, s=s, tn=tn, sn=sn: item(t, s, tn, sn, m8, u, False),
            )

            @pl.when(done)
            def _(t=t):
                finish(t)

            t, s = tn, sn
        return t, s, m8

    lax.fori_loop(0, div(count, 2), pair, (zero, zero, m8))
    o_ref[:, o_cols(0)] = o_stage[0, c]

    for tile in range(TILES):
        for k in range(2):
            @pl.when((tile != 0) | (c != k))
            def _(tile=tile, k=k):
                o_copy(jnp.int32(tile), k).wait_send()

    for j in range(4):
        for yy in range(2):
            for k in range(2):
                if j or yy or k:
                    tile = yy * 4 + ZI_OF[j]
                    first_head = rem(tz[j], KV) * GROUP + 4 * div(ys[yy], 2) + 2 * cs[k]
                    cols = pl.ds(pl.multiple_of(first_head * DH, 2 * DH), 2 * DH)
                    remote(
                        o_stage.at[tile, c], o_ref.at[:, cols], osend.at[tile, c], orecv.at[tile, cs[k]],
                        device(x, ys[yy], tz[j], cs[k]),
                    ).wait_recv()
    for copy in sends:
        copy.wait_send()
    for dz in z_order:
        for n in range(2):
            z_copy(dz, n).wait_send()
    for yy in (1, 0):
        for j in range(4):
            for k in range(2):
                if j or yy or k:
                    q_copy(j, yy, k).wait_send()


def per_device(queries, keys, values):
    hbm = pl.BlockSpec(memory_space=pl.ANY)
    dma = pltpu.SemaphoreType.DMA
    return pl.pallas_call(
        kernel,
        out_shape=pltpu.VMEM(queries.shape, queries.dtype),
        in_specs=[hbm] * 3,
        out_specs=pl.BlockSpec(memory_space=pltpu.VMEM),
        scratch_shapes=[
            pltpu.VMEM((2, 2, NZ, 8, 2, 64, DH), bf16),
            pltpu.VMEM(queries.shape, bf16),
            pltpu.VMEM(keys.shape, bf16),
            pltpu.VMEM(values.shape, bf16),
            pltpu.VMEM((TILES, 2, 64, 2 * DH), bf16),
            pltpu.VMEM((TILES, DH, 2 * DH), bf16),
            pltpu.VMEM((TILES, 2, 64, 2 * DH), bf16),
            pltpu.VMEM((TILES, 1, 2 * DH), f32),
            pltpu.VMEM((TILES, 8, 2 * DH), f32),
            pltpu.VMEM((TILES, DH, 2 * DH), f32),
            pltpu.VMEM((2, SLAB, 2 * DH), f32),
            dma((5,)),
            dma((2, NZ)), dma((2, NZ)),
            dma((16,)), dma((TILES, 2)),
            dma((36,)), dma((4, 4, 2)),
            dma((2, 8)), dma((2, 8)),
            dma((TILES, 2)), dma((TILES, 2)),
        ],
        compiler_params=pltpu.CompilerParams(
            collective_id=0, has_side_effects=True, vmem_limit_bytes=60 * 1024 * 1024
        ),
        name="regrouped_attention",
    )(queries, keys, values)


def solution(mesh):
    spec = P(("seq", "head"), None)
    return jax.shard_map(
        per_device, mesh=mesh, in_specs=(spec, spec, spec), out_specs=spec, check_vma=False
    )
```

```python
import functools
import math

import jax
import jax.numpy as jnp
from jax import lax
from jax.experimental import pallas as pl
from jax.experimental.pallas import tpu as pltpu
from jax.sharding import PartitionSpec as P

H = 32
KV = 4
DH = 128
GROUP = H // KV
NX, NY, NZ = 4, 4, 8
TILES = 8
ROUNDS = NZ // 2
SLAB = 1024
CHUNK = 256
SCALE = math.log2(math.e) / math.sqrt(DH)
ZI_OF = (0, 2, 1, 3)
f32 = jnp.float32
bf16 = jnp.bfloat16


def rem(a, b):
    return lax.rem(a, jnp.int32(b))


def div(a, b):
    return lax.div(a, jnp.int32(b))


def tie(z):
    return rem(z + 6 + 4 * rem(div(z, 2), 2), NZ)


def zsrc(z, zi):
    far = rem(z + 6 + 4 * rem(div(z, 2), 2), NZ)
    near = jnp.where(zi == 0, z, jnp.where(zi == 1, rem(z + 1, NZ), rem(z + 7, NZ)))
    return jnp.where(zi == 3, far, near)


def device(x, y, z, c):
    return (div(y, 2) * NZ + z, rem(y, 2) * 8 + x * 2 + c)


def kernel(
    q_hbm, k_hbm, v_hbm, o_ref, kv, q_own, k_own, v_own, q_in, qt, o_stage, mx, tot, acc, s_buf,
    lsem, zsend, zrecv, qsend, qrecv, gsend, grecv, csend, crecv, osend, orecv,
):
    seq = lax.axis_index("seq")
    head = lax.axis_index("head")
    yhi = div(seq, NZ)
    z = rem(seq, NZ)
    ylo = div(head, 8)
    x = rem(div(head, 2), 4)
    c = rem(head, 2)
    y = yhi * 2 + ylo
    oc = 1 - c
    oy = 3 - y
    blk = ylo * 4 + x
    kind = rem(z, KV)

    def remote(src, dst, ssem, rsem, where):
        return pltpu.make_async_remote_copy(
            src_ref=src, dst_ref=dst, send_sem=ssem, recv_sem=rsem,
            device_id=where, device_id_type=pl.DeviceIdType.MESH,
        )

    def local(src, dst, sem):
        return pltpu.make_async_copy(src, dst, sem)

    loads = [
        local(k_hbm, k_own, lsem.at[0]), local(v_hbm, v_own, lsem.at[1]), local(q_hbm, q_own, lsem.at[2]),
    ]
    for load in loads:
        load.start()

    def kv_cols(zz):
        return pl.ds(pl.multiple_of(rem(zz, KV) * DH, DH), DH)

    kept = [
        local(k_hbm.at[:, kv_cols(z)], kv.at[0, yhi, z, blk, c], lsem.at[3]),
        local(v_hbm.at[:, kv_cols(z)], kv.at[1, yhi, z, blk, c], lsem.at[4]),
    ]
    for load in kept:
        load.start()

    tz = [z, rem(z + 1, NZ), rem(z + 7, NZ), tie(z)]
    cs = (c, oc)
    ys = (y, oy)

    barrier = pltpu.get_barrier_semaphore()

    def greet(where):
        pl.semaphore_signal(barrier, inc=1, device_id=where, device_id_type=pl.DeviceIdType.MESH)

    greeted = 0
    for j in range(4):
        for yy in range(2):
            for k in range(2):
                if j or yy or k:
                    greet(device(x, ys[yy], tz[j], cs[k]))
                    greeted += 1
    for zz in (rem(z + 3, NZ), rem(z + 4, NZ), rem(z + 5, NZ), rem(2 * z + NZ - tz[3], NZ)):
        greet(device(x, y, zz, c))
        greeted += 1
    for where in (
        device(rem(x + 1, NX), y, z, c), device(rem(x + 3, NX), y, z, c), device(x, yhi * 2 + 1 - ylo, z, c),
    ):
        greet(where)
        greeted += 1

    for load in loads:
        load.wait()
    pl.semaphore_wait(barrier, greeted)

    own = (k_own, v_own)

    def z_copy(dz, n):
        zz = rem(z + dz, NZ)
        return remote(
            own[n].at[:, kv_cols(zz)], kv.at[n, yhi, z, blk, c], zsend.at[n, dz], zrecv.at[n, z], device(x, y, zz, c)
        )

    def z_landed(zz, n):
        remote(
            own[n].at[:, kv_cols(z)], kv.at[n, yhi, zz, blk, c], zsend.at[n, 0], zrecv.at[n, zz], device(x, y, zz, c)
        ).wait_recv()

    z_order = (4, 3, 5, 2, 6, 1, 7)

    def z_start():
        for dz in z_order:
            for n in range(2):
                z_copy(dz, n).start()

    for load in kept:
        load.wait()

    def q_cols(j, yy, k):
        yh = div(ys[yy], 2)
        first = rem(tz[j], KV) * GROUP + 4 * yh + 2 * cs[k]
        return pl.ds(pl.multiple_of(first * DH, 2 * DH), 2 * DH)

    def q_copy(j, yy, k):
        tile = yy * 4 + ZI_OF[j]
        return remote(
            q_own.at[:, q_cols(j, yy, k)], q_in.at[tile, c], qsend.at[(j * 2 + yy) * 2 + k], qrecv.at[tile, c],
            device(x, ys[yy], tz[j], cs[k]),
        )

    def q_landed(tile, k):
        yy, zi = divmod(tile, 4)
        zz = (z, tz[1], tz[2], tz[3])[zi]
        remote(
            q_own.at[:, pl.ds(0, 2 * DH)], q_in.at[tile, cs[k]], qsend.at[0], qrecv.at[tile, cs[k]],
            device(x, ys[yy], zz, cs[k]),
        ).wait_recv()

    def q_start():
        for yy in (1, 0):
            for j in (3, 1, 2, 0):
                for k in range(2):
                    if j or yy or k:
                        q_copy(j, yy, k).start()

    @pl.when(z < NZ // 2)
    def _():
        z_start()
        q_start()

    @pl.when(z >= NZ // 2)
    def _():
        q_start()
        z_start()

    q_in[0, c] = q_own[:, q_cols(0, 0, 0)]

    def a_dev(d):
        return device(rem(x + d * (1 - c), NX), rem(y + d * c, NY), z, c)

    def b_dev(d):
        return device(rem(x + d * c, NX), rem(y + d * (1 - c), NY), z, c)

    def block(ra, rb):
        xk = rem(x + ra * (1 - c) + rb * c, NX)
        yk = rem(y + ra * c + rb * (1 - c), NY)
        return div(yk, 2), rem(yk, 2) * 4 + xk

    def piece(r, ra, rb, n, core):
        yh, q = block(ra, rb)
        zs = pl.ds(2 * r, 2)
        if n is None:
            return kv.at[:, yh, zs, q, core]
        return kv.at[n, yh, zs, q, core]

    def g_copy(r, index, ra, rb, n, axis, d):
        ref = piece(r, ra, rb, n, c)
        to = a_dev(d % 4) if axis == 0 else b_dev(d % 4)
        there = ((ra - d) % 4, rb) if axis == 0 else (ra, (rb - d) % 4)
        return remote(ref, ref, gsend.at[r, index], grecv.at[r, there[0], there[1], n or 0], to)

    def g_landed(r, ra, rb, n):
        ref = piece(r, ra, rb, n, c)
        remote(ref, ref, gsend.at[r, 0], grecv.at[r, ra, rb, n or 0], a_dev(1)).wait_recv()

    def c_copy(r, ra, rb):
        ref = piece(r, ra, rb, None, c)
        return remote(ref, ref, csend.at[r, ra * 4 + rb], crecv.at[r], device(x, y, z, oc))

    def both_ways(ra, rb, axis):
        return [(ra, rb, None, axis, 1), (ra, rb, None, axis, -1)]

    events = [([], both_ways(0, 0, 0) + both_ways(0, 0, 1), (0, 0))]
    for d, n in ((1, 0), (-1, 1)):
        ra = -d % 4
        events.append(([(ra, 0, None)], [(ra, 0, n, 0, d)] + both_ways(ra, 0, 1), (ra, 0)))
    for d, n in ((1, 0), (-1, 1)):
        rb = -d % 4
        events.append(([(0, rb, None)], [(0, rb, n, 1, d)], (0, rb)))
    events.append(([(2, 0, 0), (2, 0, 1)], both_ways(2, 0, 1), (2, 0)))
    events.append(([(0, 2, 0), (0, 2, 1)], [], (0, 2)))
    for ra in (3, 1, 2):
        for d, n in ((1, 0), (-1, 1)):
            rb = -d % 4
            events.append(([(ra, rb, None)], [(ra, rb, n, 1, d)], (ra, rb)))
        events.append(([(ra, 2, 0), (ra, 2, 1)], [], (ra, 2)))
    when = (0, 7, 8, 9, 10, 17, 19, 14, 15, 22, 18, 20, 29, 27, 28, 37)
    every = len(events)
    span = max(when) + 1
    numbered, total_sends = [], 0
    for waits, outs, where in events:
        numbered.append((waits, [(total_sends + i, o) for i, o in enumerate(outs)], where))
        total_sends += len(outs)

    def run_event(e, r):
        waits, outs, where = numbered[e]
        if e == 0:
            for i in range(2):
                zz = 2 * r + i

                @pl.when(zz != z)
                def _(zz=zz):
                    for n in range(2):
                        z_landed(zz, n)
        for w in waits:
            g_landed(r, *w)
        for i, o in outs:
            g_copy(r, i, *o).start()
        c_copy(r, *where).start()

    by_slot = {t % every: e for e, t in enumerate(when)}

    def slot(s):
        def case(m):
            e = by_slot[m]

            def run():
                r = div(s - when[e], every)

                @pl.when((s >= when[e]) & (r < ROUNDS))
                def _():
                    run_event(e, r)

            return run

        lax.switch(rem(s, every), [case(m) for m in range(every)])

    def slots(lo, hi):
        lax.fori_loop(lo, hi, lambda s, _: (slot(s), 0)[1], 0)

    slots(0, span)

    for tile in range(TILES):
        for k in range(2):
            if tile or k:
                q_landed(tile, k)
        for h in range(2):
            part = q_in[tile, :, :, h * DH : (h + 1) * DH].reshape(2 * 64, DH)
            qt[tile, :, h * DH : (h + 1) * DH] = part.T
    mx[...] = jnp.full(mx.shape, -jnp.inf, f32)
    tot[...] = jnp.zeros(tot.shape, f32)
    acc[...] = jnp.zeros(acc.shape, f32)

    def last_slab(t):
        side = jnp.where(t < 4, yhi, 1 - yhi)
        return side * NZ + zsrc(z, rem(t, 4))

    def segment(n, s, g):
        yh = div(s, NZ)
        zz = rem(s, NZ)
        return jnp.concatenate([kv[n, yh, zz, 2 * g + i].reshape(2 * 64, DH) for i in range(2)], axis=0)

    def fold(v, op):
        return op(v.reshape(v.shape[0] // 8, 8, v.shape[1]), axis=0)

    def score(t, s, g, slot, masked):
        sc = lax.dot_general(
            segment(0, s, g), qt[t], (((1,), (0,)), ((), ())), preferred_element_type=f32
        )
        if masked:
            yl = jnp.where(t < 4, ylo, 1 - ylo)
            row = rem(lax.broadcasted_iota(jnp.int32, sc.shape, 1), 128) + (yl * 4 + x) * 128
            key = lax.broadcasted_iota(jnp.int32, sc.shape, 0) + g * CHUNK
            sc = jnp.where(key <= row, sc, -jnp.inf)
        s_buf[slot, g * CHUNK : (g + 1) * CHUNK] = sc
        return fold(sc, jnp.max)

    def apply(s, g, slot, top8, l8, pv):
        sc = s_buf[slot, g * CHUNK : (g + 1) * CHUNK].reshape(CHUNK // 8, 8, 2 * DH)
        p = jnp.exp2((sc - top8[None]) * SCALE)
        l8 = l8 + jnp.sum(p, axis=0)
        d = lax.dot_general(
            segment(1, s, g), p.reshape(CHUNK, 2 * DH).astype(bf16), (((0,), (0,)), ((), ())),
            preferred_element_type=f32,
        )
        return l8, (d if pv is None else pv + d)

    parts = SLAB // CHUNK

    def o_cols(t):
        return pl.ds(pl.multiple_of((kind * GROUP + 4 * yhi + 2 * c) * DH, 2 * DH), 2 * DH)

    def o_copy(t, k):
        cc = k
        yy = jnp.where(t < 4, y, oy)
        zz = zsrc(z, rem(t, 4))
        return remote(
            o_stage.at[t, cc], o_ref.at[:, o_cols(t)], osend.at[t, cc],
            orecv.at[t, c], device(x, yy, zz, cc),
        )

    def finish(t):
        for h in range(2):
            cols = slice(h * DH, (h + 1) * DH)
            whole = jnp.sum(tot[t, :, cols], axis=0, keepdims=True)
            rows = (acc[t, :, cols] / whole).T.astype(bf16)
            o_stage[t, :, :, cols] = rows.reshape(2, 64, DH)

        for k in range(2):
            @pl.when((t != 0) | (c != k))
            def _():
                o_copy(t, k).start()

    def prep(t, m8):
        old = mx[t]
        top = jnp.maximum(old, jnp.max(m8, axis=0, keepdims=True))
        factor = jnp.exp2((old - top) * SCALE)
        mx[t] = top
        return jnp.broadcast_to(top, (8, 2 * DH)), factor

    def item(t, s, tn, sn, m8, u, masked):
        top8, factor = prep(t, m8)
        l8, pv, nm = tot[t] * factor, None, None
        for g in range(parts):
            r = score(tn, sn, g, 1 - u, masked)
            nm = r if nm is None else jnp.maximum(nm, r)
            l8, pv = apply(s, g, u, top8, l8, pv)
        acc[t] = acc[t] * factor + pv
        tot[t] = l8
        return nm

    near = [zsrc(z, i) for i in range(4)]

    def pick(i):
        zq = near[3]
        for k in (2, 1, 0):
            zq = jnp.where(i == k, near[k], zq)
        return zq

    def tile_at(u):
        return rem(u + 4 * yhi, TILES)

    def steps(u, r):
        zq = pick(rem(u, 4))
        own_side = jnp.clip(zq - 2 * r + 1, 0, 2)
        return own_side + jnp.where(u >= 4, 2, 0)

    def following(u, r):
        at = jnp.int32(4)
        for k in (3, 2, 1, 0):
            at = jnp.where((k > u) & (steps(jnp.int32(k), r) > 0), k, at)
        return jnp.where(u >= 4, u + 1, at)

    def slab_of(i, r):
        return div(i, 2) * NZ + 2 * r + rem(i, 2)

    def first(t, s, masked):
        m8 = None
        for g in range(parts):
            v = score(t, s, g, 0, masked)
            m8 = v if m8 is None else jnp.maximum(m8, v)
        return m8

    def one_round(r, _):
        ref = kv.at[:, :, pl.ds(2 * r, 2), :, oc]
        remote(ref, ref, csend.at[r, 0], crecv.at[r], device(x, y, z, oc)).wait_recv()
        u0 = following(jnp.int32(-1), r)
        t0 = tile_at(u0)
        s0 = slab_of(jnp.int32(0), r)
        m8 = lax.cond(s0 == last_slab(t0), lambda: first(t0, s0, True), lambda: first(t0, s0, False))
        count = jnp.int32(0)
        for k in range(TILES):
            count = count + steps(jnp.int32(k), r)
        base = span + every * r

        def pair(i, carry):
            u, k, m8 = carry
            slots(lax.min(base + 2 * i, base + every), lax.min(base + 2 * i + 2, base + every))
            for h in range(2):
                t, s = tile_at(u), slab_of(k, r)
                done = k + 1 == steps(u, r)
                un = jnp.where(done, following(u, r), u)
                kn = jnp.where(done, 0, k + 1)
                over = un >= TILES
                tn = jnp.where(over, t, tile_at(un))
                sn = jnp.where(over, s, slab_of(kn, r))
                live = u < TILES
                masked = jnp.where(sn == last_slab(tn), 1, 0)
                m8 = lax.switch(
                    jnp.where(live, masked, 2),
                    [
                        lambda m8=m8, h=h, a=(t, s, tn, sn): item(*a, m8, h, False),
                        lambda m8=m8, h=h, a=(t, s, tn, sn): item(*a, m8, h, True),
                        lambda m8=m8: m8,
                    ],
                )
                final = jnp.where(u >= 4, ROUNDS - 1, div(pick(rem(u, 4)), 2))

                @pl.when(live & done & (r == final))
                def _(t=t):
                    finish(t)

                u, k = un, kn
            return u, k, m8

        pairs = div(count + 1, 2)
        lax.fori_loop(0, pairs, pair, (u0, jnp.int32(0), m8))
        slots(lax.min(base + 2 * pairs, base + every), base + every)
        return 0

    lax.fori_loop(0, ROUNDS, one_round, 0)
    o_ref[:, o_cols(0)] = o_stage[0, c]

    for tile in range(TILES):
        for k in range(2):
            @pl.when((tile != 0) | (c != k))
            def _(tile=tile, k=k):
                o_copy(jnp.int32(tile), k).wait_send()

    for j in range(4):
        for yy in range(2):
            for k in range(2):
                if j or yy or k:
                    tile = yy * 4 + ZI_OF[j]
                    first_head = rem(tz[j], KV) * GROUP + 4 * div(ys[yy], 2) + 2 * cs[k]
                    cols = pl.ds(pl.multiple_of(first_head * DH, 2 * DH), 2 * DH)
                    remote(
                        o_stage.at[tile, c], o_ref.at[:, cols], osend.at[tile, c], orecv.at[tile, cs[k]],
                        device(x, ys[yy], tz[j], cs[k]),
                    ).wait_recv()

    def sent(r, _):
        for _, outs, where in numbered:
            for i, o in outs:
                g_copy(r, i, *o).wait_send()
            c_copy(r, *where).wait_send()
        return 0

    lax.fori_loop(0, ROUNDS, sent, 0)
    for dz in z_order:
        for n in range(2):
            z_copy(dz, n).wait_send()
    for yy in (1, 0):
        for j in range(4):
            for k in range(2):
                if j or yy or k:
                    q_copy(j, yy, k).wait_send()


def per_device(queries, keys, values):
    hbm = pl.BlockSpec(memory_space=pl.ANY)
    dma = pltpu.SemaphoreType.DMA
    return pl.pallas_call(
        kernel,
        out_shape=pltpu.VMEM(queries.shape, queries.dtype),
        in_specs=[hbm] * 3,
        out_specs=pl.BlockSpec(memory_space=pltpu.VMEM),
        scratch_shapes=[
            pltpu.VMEM((2, 2, NZ, 8, 2, 64, DH), bf16),
            pltpu.VMEM(queries.shape, bf16),
            pltpu.VMEM(keys.shape, bf16),
            pltpu.VMEM(values.shape, bf16),
            pltpu.VMEM((TILES, 2, 64, 2 * DH), bf16),
            pltpu.VMEM((TILES, DH, 2 * DH), bf16),
            pltpu.VMEM((TILES, 2, 64, 2 * DH), bf16),
            pltpu.VMEM((TILES, 1, 2 * DH), f32),
            pltpu.VMEM((TILES, 8, 2 * DH), f32),
            pltpu.VMEM((TILES, DH, 2 * DH), f32),
            pltpu.VMEM((2, SLAB, 2 * DH), f32),
            dma((5,)),
            dma((2, NZ)), dma((2, NZ)),
            dma((16,)), dma((TILES, 2)),
            dma((ROUNDS, 20)), dma((ROUNDS, 4, 4, 2)),
            dma((ROUNDS, 16)), dma((ROUNDS,)),
            dma((TILES, 2)), dma((TILES, 2)),
        ],
        compiler_params=pltpu.CompilerParams(
            collective_id=0, has_side_effects=True, vmem_limit_bytes=60 * 1024 * 1024
        ),
        name="regrouped_attention",
    )(queries, keys, values)


def solution(mesh):
    spec = P(("seq", "head"), None)
    return jax.shard_map(
        per_device, mesh=mesh, in_specs=(spec, spec, spec), out_specs=spec, check_vma=False
    )
```

```python
import functools
import math

import jax
import jax.numpy as jnp
from jax import lax
from jax.experimental import pallas as pl
from jax.experimental.pallas import tpu as pltpu
from jax.sharding import PartitionSpec as P

H = 32
KV = 4
DH = 128
GROUP = H // KV
NX, NY, NZ = 4, 4, 8
TILES = 8
SLAB = 1024
CHUNK = 256
BLOCKS = NX * NY
PACE = 2
SCALE = math.log2(math.e) / math.sqrt(DH)
ZI_OF = (0, 2, 1, 3)
f32 = jnp.float32
bf16 = jnp.bfloat16


def rem(a, b):
    return lax.rem(a, jnp.int32(b))


def div(a, b):
    return lax.div(a, jnp.int32(b))


def tie(z):
    return rem(z + 6 + 4 * rem(div(z, 2), 2), NZ)


def zsrc(z, zi):
    far = rem(z + 6 + 4 * rem(div(z, 2), 2), NZ)
    near = jnp.where(zi == 0, z, jnp.where(zi == 1, rem(z + 1, NZ), rem(z + 7, NZ)))
    return jnp.where(zi == 3, far, near)


def device(x, y, z, c):
    return (div(y, 2) * NZ + z, rem(y, 2) * 8 + x * 2 + c)


def kernel(
    q_hbm, k_hbm, v_hbm, o_ref, kv, q_own, k_own, v_own, q_in, qt, o_stage, mx, tot, acc, s_buf,
    lsem, zsend, zrecv, qsend, qrecv, gsend, grecv, csend, crecv, osend, orecv,
):
    seq = lax.axis_index("seq")
    head = lax.axis_index("head")
    yhi = div(seq, NZ)
    z = rem(seq, NZ)
    ylo = div(head, 8)
    x = rem(div(head, 2), 4)
    c = rem(head, 2)
    y = yhi * 2 + ylo
    oc = 1 - c
    oy = 3 - y
    blk = ylo * 4 + x
    kind = rem(z, KV)

    def remote(src, dst, ssem, rsem, where):
        return pltpu.make_async_remote_copy(
            src_ref=src, dst_ref=dst, send_sem=ssem, recv_sem=rsem,
            device_id=where, device_id_type=pl.DeviceIdType.MESH,
        )

    def local(src, dst, sem):
        return pltpu.make_async_copy(src, dst, sem)

    loads = [
        local(k_hbm, k_own, lsem.at[0]), local(v_hbm, v_own, lsem.at[1]), local(q_hbm, q_own, lsem.at[2]),
    ]
    for load in loads:
        load.start()

    def kv_cols(zz):
        return pl.ds(pl.multiple_of(rem(zz, KV) * DH, DH), DH)

    kept = [
        local(k_hbm.at[:, kv_cols(z)], kv.at[0, yhi, z, blk, c], lsem.at[3]),
        local(v_hbm.at[:, kv_cols(z)], kv.at[1, yhi, z, blk, c], lsem.at[4]),
    ]
    for load in kept:
        load.start()

    tz = [z, rem(z + 1, NZ), rem(z + 7, NZ), tie(z)]
    cs = (c, oc)
    ys = (y, oy)

    barrier = pltpu.get_barrier_semaphore()

    def greet(where):
        pl.semaphore_signal(barrier, inc=1, device_id=where, device_id_type=pl.DeviceIdType.MESH)

    greeted = 0
    for j in range(4):
        for yy in range(2):
            for k in range(2):
                if j or yy or k:
                    greet(device(x, ys[yy], tz[j], cs[k]))
                    greeted += 1
    for zz in (rem(z + 3, NZ), rem(z + 4, NZ), rem(z + 5, NZ), rem(2 * z + NZ - tz[3], NZ)):
        greet(device(x, y, zz, c))
        greeted += 1
    for where in (
        device(rem(x + 1, NX), y, z, c), device(rem(x + 3, NX), y, z, c), device(x, yhi * 2 + 1 - ylo, z, c),
    ):
        greet(where)
        greeted += 1

    for load in loads:
        load.wait()
    pl.semaphore_wait(barrier, greeted)

    own = (k_own, v_own)

    def z_copy(dz, n):
        zz = rem(z + dz, NZ)
        return remote(
            own[n].at[:, kv_cols(zz)], kv.at[n, yhi, z, blk, c], zsend.at[n, dz], zrecv.at[n, z], device(x, y, zz, c)
        )

    def z_landed(zz, n):
        remote(
            own[n].at[:, kv_cols(z)], kv.at[n, yhi, zz, blk, c], zsend.at[n, 0], zrecv.at[n, zz], device(x, y, zz, c)
        ).wait_recv()

    z_order = (4, 3, 5, 2, 6, 1, 7)

    def z_start():
        for dz in z_order:
            for n in range(2):
                z_copy(dz, n).start()

    for load in kept:
        load.wait()

    def q_cols(j, yy, k):
        yh = div(ys[yy], 2)
        first = rem(tz[j], KV) * GROUP + 4 * yh + 2 * cs[k]
        return pl.ds(pl.multiple_of(first * DH, 2 * DH), 2 * DH)

    def q_copy(j, yy, k):
        tile = yy * 4 + ZI_OF[j]
        return remote(
            q_own.at[:, q_cols(j, yy, k)], q_in.at[tile, c], qsend.at[(j * 2 + yy) * 2 + k], qrecv.at[tile, c],
            device(x, ys[yy], tz[j], cs[k]),
        )

    def q_landed(tile, k):
        yy, zi = divmod(tile, 4)
        zz = (z, tz[1], tz[2], tz[3])[zi]
        remote(
            q_own.at[:, pl.ds(0, 2 * DH)], q_in.at[tile, cs[k]], qsend.at[0], qrecv.at[tile, cs[k]],
            device(x, ys[yy], zz, cs[k]),
        ).wait_recv()

    def q_start():
        for yy in (1, 0):
            for j in (3, 1, 2, 0):
                for k in range(2):
                    if j or yy or k:
                        q_copy(j, yy, k).start()

    z_start()
    q_start()

    q_in[0, c] = q_own[:, q_cols(0, 0, 0)]

    din = 1 + 2 * rem(y, 2)
    dys = (0, din, NY - din, 2)
    IN, OUT, FAR = 1, 2, 3
    XUP, XDOWN, YIN, YOUT = range(4)
    to = (
        device(rem(x + 1, NX), y, z, c), device(rem(x + 3, NX), y, z, c),
        device(x, rem(y + dys[IN], NY), z, c), device(x, rem(y + dys[OUT], NY), z, c),
    )
    order = (
        (0, 0), (3, 0), (1, 0), (0, IN), (0, OUT), (2, 0), (3, IN), (1, IN),
        (3, OUT), (1, OUT), (2, IN), (2, OUT), (0, FAR), (3, FAR), (1, FAR), (2, FAR),
    )

    def block(dx, dy):
        xk = rem(x + dx, NX)
        yk = rem(y + dy, NY)
        return div(yk, 2), rem(yk, 2) * 4 + xk

    def piece(dx, sy, n, core):
        yh, q = block(dx, dys[sy])
        if n is None:
            return kv.at[:, yh, :, q, core]
        return kv.at[n, yh, :, q, core]

    def plan(core):
        made = {}
        for dx, sy in order:
            outs = []
            if (dx, sy) == (0, 0):
                outs += [(None, XUP, (3, 0)), (None, XDOWN, (1, 0)), (None, YIN, (0, IN)), (None, YOUT, (0, OUT))]
            if dx in (3, 1) and (core == 1 or sy == 0):
                outs.append((0, XUP, (2, sy)) if dx == 3 else (1, XDOWN, (2, sy)))
            if core == 0 and sy == 0 and dx:
                outs += [(None, YIN, (dx, IN)), (None, YOUT, (dx, OUT))]
            if core == 1 and dx == 0 and sy:
                outs += [(None, XUP, (3, sy)), (None, XDOWN, (1, sy))]
            if (core == 0 or dx == 0) and sy in (IN, OUT):
                outs.append((0, YOUT, (dx, FAR)) if sy == IN else (1, YIN, (dx, FAR)))
            if core == 0:
                halves = sy == FAR or (dx, sy) == (2, 0)
            else:
                halves = dx == 2 or (dx, sy) == (0, FAR)
            made[dx, sy] = (halves, outs)
        return made

    def g_copy(where, i, n, via, there):
        ref = piece(*where, n, c)
        return remote(ref, ref, gsend.at[i], grecv.at[there[0], there[1], n or 0], to[via])

    def g_copies(core):
        found, i = {}, 0
        for where, (halves, outs) in plan(core).items():
            found[where] = (halves, [])
            for n, via, there in outs:
                found[where][1].append((i, n, via, there))
                i += 1
        return found

    def c_copy(p):
        ref = piece(*order[p], None, c)
        return remote(ref, ref, csend.at[p], crecv.at[p], device(x, y, z, oc))

    def event(p):
        where = order[p]
        for core in range(2):
            @pl.when(c == core)
            def _(core=core):
                halves, outs = g_copies(core)[where]
                if p:
                    for n in (0, 1) if halves else (None,):
                        ref = piece(*where, n, c)
                        remote(ref, ref, gsend.at[0], grecv.at[where[0], where[1], n or 0], to[0]).wait_recv()
                for out in outs:
                    g_copy(where, *out).start()
        c_copy(p).start()

    for dz in range(1, NZ):
        for n in range(2):
            z_landed(rem(z + dz, NZ), n)

    def take_queries():
        for tile in range(TILES):
            for k in range(2):
                if tile or k:
                    q_landed(tile, k)
            for h in range(2):
                part = q_in[tile, :, :, h * DH : (h + 1) * DH].reshape(2 * 64, DH)
                qt[tile, :, h * DH : (h + 1) * DH] = part.T

    mx[...] = jnp.full(mx.shape, -jnp.inf, f32)
    tot[...] = jnp.zeros(tot.shape, f32)
    acc[...] = jnp.zeros(acc.shape, f32)

    def last_slab(t):
        side = jnp.where(t < 4, yhi, 1 - yhi)
        return side * NZ + zsrc(z, rem(t, 4))

    def segment(n, at, g):
        yh, z0, dz, q0, dq = at
        rows = []
        for i in range(2 * g, 2 * g + 2):
            rows.append(kv[n, yh, z0 + i * dz, q0 + i * dq].reshape(2 * 64, DH))
        return jnp.concatenate(rows, axis=0)

    def fold(v, op):
        return op(v.reshape(v.shape[0] // 8, 8, v.shape[1]), axis=0)

    def score(t, s, g, slot, masked):
        sc = lax.dot_general(
            segment(0, s, g), qt[t], (((1,), (0,)), ((), ())), preferred_element_type=f32
        )
        if masked:
            yl = jnp.where(t < 4, ylo, 1 - ylo)
            row = rem(lax.broadcasted_iota(jnp.int32, sc.shape, 1), 128) + (yl * 4 + x) * 128
            key = lax.broadcasted_iota(jnp.int32, sc.shape, 0) + g * CHUNK
            sc = jnp.where(key <= row, sc, -jnp.inf)
        s_buf[slot, g * CHUNK : (g + 1) * CHUNK] = sc
        return fold(sc, jnp.max)

    def apply(s, g, slot, top8, l8, pv):
        sc = s_buf[slot, g * CHUNK : (g + 1) * CHUNK].reshape(CHUNK // 8, 8, 2 * DH)
        p = jnp.exp2((sc - top8[None]) * SCALE)
        l8 = l8 + jnp.sum(p, axis=0)
        d = lax.dot_general(
            segment(1, s, g), p.reshape(CHUNK, 2 * DH).astype(bf16), (((0,), (0,)), ((), ())),
            preferred_element_type=f32,
        )
        return l8, (d if pv is None else pv + d)

    parts = SLAB // CHUNK

    def o_cols(t):
        return pl.ds(pl.multiple_of((kind * GROUP + 4 * yhi + 2 * c) * DH, 2 * DH), 2 * DH)

    def o_copy(t, k):
        cc = k
        yy = jnp.where(t < 4, y, oy)
        zz = zsrc(z, rem(t, 4))
        return remote(
            o_stage.at[t, cc], o_ref.at[:, o_cols(t)], osend.at[t, cc],
            orecv.at[t, c], device(x, yy, zz, cc),
        )

    def finish(t):
        for h in range(2):
            cols = slice(h * DH, (h + 1) * DH)
            whole = jnp.sum(tot[t, :, cols], axis=0, keepdims=True)
            rows = (acc[t, :, cols] / whole).T.astype(bf16)
            o_stage[t, :, :, cols] = rows.reshape(2, 64, DH)

        for k in range(2):
            @pl.when((t != 0) | (c != k))
            def _():
                o_copy(t, k).start()

    def prep(t, m8):
        old = mx[t]
        top = jnp.maximum(old, jnp.max(m8, axis=0, keepdims=True))
        factor = jnp.exp2((old - top) * SCALE)
        mx[t] = top
        return jnp.broadcast_to(top, (8, 2 * DH)), factor

    def item(t, s, tn, sn, m8, u, masked):
        top8, factor = prep(t, m8)
        l8, pv, nm = tot[t] * factor, None, None
        for g in range(parts):
            r = score(tn, sn, g, 1 - u, masked)
            nm = r if nm is None else jnp.maximum(nm, r)
            l8, pv = apply(s, g, u, top8, l8, pv)
        acc[t] = acc[t] * factor + pv
        tot[t] = l8
        return nm

    near = [zsrc(z, i) for i in range(4)]

    def choose(i, values):
        got = jnp.int32(values[-1])
        for k in range(len(values) - 1):
            got = jnp.where(i == k, values[k], got)
        return got

    def cross_address(p):
        dx = choose(p, [dx for dx, _ in order])
        sy = choose(p, [sy for _, sy in order])
        yh, q = block(dx, choose(sy, dys))
        return yh, jnp.int32(0), jnp.int32(1), q, jnp.int32(0)

    late_start = 4 * yhi
    late = 4 * (1 - yhi)

    def first(t, at, masked):
        m8 = None
        for g in range(parts):
            v = score(t, at, g, 0, masked)
            m8 = v if m8 is None else jnp.maximum(m8, v)
        return m8

    def other(p):
        yh, q = block(choose(p, [dx for dx, _ in order]), choose(choose(p, [sy for _, sy in order]), dys))
        ref = kv.at[:, yh, :, q, oc]
        remote(ref, ref, csend.at[p], crecv.at[p], device(x, y, z, oc)).wait_recv()

    def relay(lo, hi):
        def step(p, _):
            lax.switch(p, [functools.partial(event, i) for i in range(BLOCKS)])
            return 0

        lax.fori_loop(lo, hi, step, 0)

    def others(lo, hi):
        lax.fori_loop(lo, hi, lambda p, _: (other(p), 0)[1], 0)

    relay(0, 5)
    take_queries()
    others(0, 5)

    def about(p):
        dx = choose(p, [dx for dx, _ in order])
        sy = choose(p, [sy for _, sy in order])
        _, q = block(dx, choose(sy, dys))
        early = jnp.where(yhi == 0, sy < 2, sy >= 2)
        nc = jnp.where((p < 16) & early, 4, 0)
        far_turn = p >= 16
        own_turn = (p >= 10) & (p < 14)
        ts = jnp.where(far_turn, 23 - p, jnp.where(own_turn, p - 10, 0))
        slabs = jnp.where(far_turn | own_turn, choose(rem(ts, 4), near) + 1, 0)
        return p, nc, q, ts, nc + slabs

    def after(p):
        skip = jnp.where(
            yhi == 0, jnp.where((p == 7) | (p == 13), 3, jnp.where(p == 3, 2, 1)), jnp.where(p == 4, 4, 1)
        )
        return p + skip

    def what(k, stage):
        p, nc, q, ts, n = stage
        crosses = k < nc
        t = jnp.where(crosses, late + k, ts)
        side = jnp.where(ts < 4, yhi, 1 - yhi)
        dz = jnp.where(crosses, 1, 0)
        at = (
            jnp.where(crosses, 0, side), jnp.where(crosses, 0, k - nc), dz, jnp.where(crosses, q, 0), 1 - dz,
        )
        return t, at, (k + 1 == n) & (n != nc)

    zero = jnp.int32(0)
    stage0 = about(late_start)
    t0, at0, _ = what(zero, stage0)
    m8 = first(t0, at0, False)
    total = 40 + 2 * (near[0] + near[1] + near[2] + near[3])

    def advance(i, stage, ran, had):
        p = stage[0]
        pn = lax.min(after(p), 19)
        due = lax.max(ran, lax.min(lax.max(5 + div(i, PACE), pn + 1), BLOCKS))
        relay(ran, due)
        seen = lax.max(had, lax.min(pn + 1, BLOCKS))
        others(had, seen)
        return about(pn), due, seen

    def ended(p, ts):
        @pl.when((p >= 16) | ((p >= 10) & (p < 14) & (yhi == 0)))
        def _():
            finish(ts)

        @pl.when((p == 15) & (yhi == 1))
        def _():
            lax.fori_loop(0, 4, lambda t, _: (finish(t), 0)[1], 0)

    def pair(i, carry):
        k, stage, ran, had, t, at, m8 = carry
        for h in range(2):
            last = k + 1 == stage[4]
            more, ran, had = lax.cond(
                last,
                lambda stage=stage, ran=ran, had=had: advance(i, stage, ran, had),
                lambda stage=stage, ran=ran, had=had: (stage, ran, had),
            )
            kn = jnp.where(last, 0, k + 1)
            tn, an, diag = what(kn, more)
            m8 = lax.cond(
                diag,
                lambda m8=m8, h=h, a=(t, at, tn, an): item(*a, m8, h, True),
                lambda m8=m8, h=h, a=(t, at, tn, an): item(*a, m8, h, False),
            )

            @pl.when(last)
            def _(stage=stage):
                ended(stage[0], stage[3])

            k, stage, t, at = kn, more, tn, an
        return k, stage, ran, had, t, at, m8

    lax.fori_loop(0, div(total, 2), pair, (zero, stage0, zero + 5, zero + 5, t0, at0, m8))
    o_ref[:, o_cols(0)] = o_stage[0, c]

    for tile in range(TILES):
        for k in range(2):
            @pl.when((tile != 0) | (c != k))
            def _(tile=tile, k=k):
                o_copy(jnp.int32(tile), k).wait_send()

    for j in range(4):
        for yy in range(2):
            for k in range(2):
                if j or yy or k:
                    tile = yy * 4 + ZI_OF[j]
                    first_head = rem(tz[j], KV) * GROUP + 4 * div(ys[yy], 2) + 2 * cs[k]
                    cols = pl.ds(pl.multiple_of(first_head * DH, 2 * DH), 2 * DH)
                    remote(
                        o_stage.at[tile, c], o_ref.at[:, cols], osend.at[tile, c], orecv.at[tile, cs[k]],
                        device(x, ys[yy], tz[j], cs[k]),
                    ).wait_recv()

    for core in range(2):
        @pl.when(c == core)
        def _(core=core):
            for where, (_, outs) in g_copies(core).items():
                for out in outs:
                    g_copy(where, *out).wait_send()

    for p in range(len(order)):
        c_copy(p).wait_send()
    for dz in z_order:
        for n in range(2):
            z_copy(dz, n).wait_send()
    for yy in (1, 0):
        for j in range(4):
            for k in range(2):
                if j or yy or k:
                    q_copy(j, yy, k).wait_send()


def per_device(queries, keys, values):
    hbm = pl.BlockSpec(memory_space=pl.ANY)
    dma = pltpu.SemaphoreType.DMA
    return pl.pallas_call(
        kernel,
        out_shape=pltpu.VMEM(queries.shape, queries.dtype),
        in_specs=[hbm] * 3,
        out_specs=pl.BlockSpec(memory_space=pltpu.VMEM),
        scratch_shapes=[
            pltpu.VMEM((2, 2, NZ, 8, 2, 64, DH), bf16),
            pltpu.VMEM(queries.shape, bf16),
            pltpu.VMEM(keys.shape, bf16),
            pltpu.VMEM(values.shape, bf16),
            pltpu.VMEM((TILES, 2, 64, 2 * DH), bf16),
            pltpu.VMEM((TILES, DH, 2 * DH), bf16),
            pltpu.VMEM((TILES, 2, 64, 2 * DH), bf16),
            pltpu.VMEM((TILES, 1, 2 * DH), f32),
            pltpu.VMEM((TILES, 8, 2 * DH), f32),
            pltpu.VMEM((TILES, DH, 2 * DH), f32),
            pltpu.VMEM((2, SLAB, 2 * DH), f32),
            dma((5,)),
            dma((2, NZ)), dma((2, NZ)),
            dma((16,)), dma((TILES, 2)),
            dma((24,)), dma((4, 4, 2)),
            dma((16,)), dma((16,)),
            dma((TILES, 2)), dma((TILES, 2)),
        ],
        compiler_params=pltpu.CompilerParams(
            collective_id=0, has_side_effects=True, vmem_limit_bytes=60 * 1024 * 1024
        ),
        name="regrouped_attention",
    )(queries, keys, values)


def solution(mesh):
    spec = P(("seq", "head"), None)
    return jax.shard_map(
        per_device, mesh=mesh, in_specs=(spec, spec, spec), out_specs=spec, check_vma=False
    )
```

```python
import functools
import math

import jax
import jax.numpy as jnp
from jax import lax
from jax.experimental import pallas as pl
from jax.experimental.pallas import tpu as pltpu
from jax.sharding import PartitionSpec as P

H = 32
KV = 4
DH = 128
GROUP = H // KV
NX, NY, NZ = 4, 4, 8
TILES = 8
SLAB = 1024
CHUNK = 512
BLOCKS = NX * NY
PACE = 1
FIRST = 5
SCALE = math.log2(math.e) / math.sqrt(DH)
ZI_OF = (0, 2, 1, 3)
f32 = jnp.float32
bf16 = jnp.bfloat16


def rem(a, b):
    return lax.rem(a, jnp.int32(b))


def div(a, b):
    return lax.div(a, jnp.int32(b))


def tie(z):
    return rem(z + 6 + 4 * rem(div(z, 2), 2), NZ)


def zsrc(z, zi):
    far = rem(z + 6 + 4 * rem(div(z, 2), 2), NZ)
    near = jnp.where(zi == 0, z, jnp.where(zi == 1, rem(z + 1, NZ), rem(z + 7, NZ)))
    return jnp.where(zi == 3, far, near)


def device(x, y, z, c):
    return (div(y, 2) * NZ + z, rem(y, 2) * 8 + x * 2 + c)


def kernel(
    q_hbm, k_hbm, v_hbm, o_ref, kv, q_own, k_own, v_own, q_in, qt, o_stage, mx, tot, acc, s_buf,
    lsem, zsend, zrecv, qsend, qrecv, gsend, grecv, csend, crecv, osend, orecv,
):
    seq = lax.axis_index("seq")
    head = lax.axis_index("head")
    yhi = div(seq, NZ)
    z = rem(seq, NZ)
    ylo = div(head, 8)
    x = rem(div(head, 2), 4)
    c = rem(head, 2)
    y = yhi * 2 + ylo
    oc = 1 - c
    oy = 3 - y
    blk = ylo * 4 + x
    kind = rem(z, KV)

    def remote(src, dst, ssem, rsem, where):
        return pltpu.make_async_remote_copy(
            src_ref=src, dst_ref=dst, send_sem=ssem, recv_sem=rsem,
            device_id=where, device_id_type=pl.DeviceIdType.MESH,
        )

    def local(src, dst, sem):
        return pltpu.make_async_copy(src, dst, sem)

    loads = [
        local(k_hbm, k_own, lsem.at[0]), local(v_hbm, v_own, lsem.at[1]), local(q_hbm, q_own, lsem.at[2]),
    ]
    for load in loads:
        load.start()

    def kv_cols(zz):
        return pl.ds(pl.multiple_of(rem(zz, KV) * DH, DH), DH)

    kept = [
        local(k_hbm.at[:, kv_cols(z)], kv.at[0, yhi, z, blk, c], lsem.at[3]),
        local(v_hbm.at[:, kv_cols(z)], kv.at[1, yhi, z, blk, c], lsem.at[4]),
    ]
    for load in kept:
        load.start()

    tz = [z, rem(z + 1, NZ), rem(z + 7, NZ), tie(z)]
    cs = (c, oc)
    ys = (y, oy)

    barrier = pltpu.get_barrier_semaphore()

    def greet(where):
        pl.semaphore_signal(barrier, inc=1, device_id=where, device_id_type=pl.DeviceIdType.MESH)

    greeted = 0
    for j in range(4):
        for yy in range(2):
            for k in range(2):
                if j or yy or k:
                    greet(device(x, ys[yy], tz[j], cs[k]))
                    greeted += 1
    for zz in (rem(z + 3, NZ), rem(z + 4, NZ), rem(z + 5, NZ), rem(2 * z + NZ - tz[3], NZ)):
        greet(device(x, y, zz, c))
        greeted += 1
    for where in (
        device(rem(x + 1, NX), y, z, c), device(rem(x + 3, NX), y, z, c), device(x, yhi * 2 + 1 - ylo, z, c),
    ):
        greet(where)
        greeted += 1

    for load in loads:
        load.wait()
    pl.semaphore_wait(barrier, greeted)

    own = (k_own, v_own)

    def z_copy(dz, n):
        zz = rem(z + dz, NZ)
        return remote(
            own[n].at[:, kv_cols(zz)], kv.at[n, yhi, z, blk, c], zsend.at[n, dz], zrecv.at[n, z], device(x, y, zz, c)
        )

    def z_landed(zz, n):
        remote(
            own[n].at[:, kv_cols(z)], kv.at[n, yhi, zz, blk, c], zsend.at[n, 0], zrecv.at[n, zz], device(x, y, zz, c)
        ).wait_recv()

    z_order = (4, 3, 5, 2, 6, 1, 7)

    def z_start():
        for dz in z_order:
            for n in range(2):
                z_copy(dz, n).start()

    for load in kept:
        load.wait()

    def q_cols(j, yy, k):
        yh = div(ys[yy], 2)
        first = rem(tz[j], KV) * GROUP + 4 * yh + 2 * cs[k]
        return pl.ds(pl.multiple_of(first * DH, 2 * DH), 2 * DH)

    def q_copy(j, yy, k):
        tile = yy * 4 + ZI_OF[j]
        return remote(
            q_own.at[:, q_cols(j, yy, k)], q_in.at[tile, c], qsend.at[(j * 2 + yy) * 2 + k], qrecv.at[tile, c],
            device(x, ys[yy], tz[j], cs[k]),
        )

    def q_landed(tile, k):
        yy, zi = divmod(tile, 4)
        zz = (z, tz[1], tz[2], tz[3])[zi]
        remote(
            q_own.at[:, pl.ds(0, 2 * DH)], q_in.at[tile, cs[k]], qsend.at[0], qrecv.at[tile, cs[k]],
            device(x, ys[yy], zz, cs[k]),
        ).wait_recv()

    def q_start():
        for yy in (1, 0):
            for j in (3, 1, 2, 0):
                for k in range(2):
                    if j or yy or k:
                        q_copy(j, yy, k).start()

    z_start()
    q_start()

    q_in[0, c] = q_own[:, q_cols(0, 0, 0)]

    din = 1 + 2 * rem(y, 2)
    dys = (0, din, NY - din, 2)
    IN, OUT, FAR = 1, 2, 3
    XUP, XDOWN, YIN, YOUT = range(4)
    to = (
        device(rem(x + 1, NX), y, z, c), device(rem(x + 3, NX), y, z, c),
        device(x, rem(y + dys[IN], NY), z, c), device(x, rem(y + dys[OUT], NY), z, c),
    )
    orders = (
        (
            (0, 0), (3, 0), (1, 0), (0, IN), (2, 0), (3, IN), (1, IN), (0, OUT),
            (2, IN), (3, OUT), (1, OUT), (2, OUT), (0, FAR), (3, FAR), (1, FAR), (2, FAR),
        ),
        (
            (0, 0), (0, OUT), (3, 0), (1, 0), (3, OUT), (1, OUT), (0, IN), (0, FAR),
            (2, 0), (2, OUT), (3, FAR), (1, FAR), (2, FAR), (3, IN), (1, IN), (2, IN),
        ),
    )

    def block(dx, dy):
        xk = rem(x + dx, NX)
        yk = rem(y + dy, NY)
        return div(yk, 2), rem(yk, 2) * 4 + xk

    def piece(dx, sy, n, core):
        yh, q = block(dx, dys[sy])
        if n is None:
            return kv.at[:, yh, :, q, core]
        return kv.at[n, yh, :, q, core]

    def plan(core):
        made = {}
        for dx, sy in orders[0]:
            outs = []
            if (dx, sy) == (0, 0):
                outs += [(None, XUP, (3, 0)), (None, XDOWN, (1, 0)), (None, YIN, (0, IN)), (None, YOUT, (0, OUT))]
            if dx in (3, 1) and (core == 1 or sy == 0):
                outs.append((0, XUP, (2, sy)) if dx == 3 else (1, XDOWN, (2, sy)))
            if core == 0 and sy == 0 and dx:
                outs += [(None, YIN, (dx, IN)), (None, YOUT, (dx, OUT))]
            if core == 1 and dx == 0 and sy:
                outs += [(None, XUP, (3, sy)), (None, XDOWN, (1, sy))]
            if (core == 0 or dx == 0) and sy in (IN, OUT):
                outs.append((0, YOUT, (dx, FAR)) if sy == IN else (1, YIN, (dx, FAR)))
            if core == 0:
                halves = sy == FAR or (dx, sy) == (2, 0)
            else:
                halves = dx == 2 or (dx, sy) == (0, FAR)
            made[dx, sy] = (halves, outs)
        return made

    def g_copy(where, i, n, via, there):
        ref = piece(*where, n, c)
        return remote(ref, ref, gsend.at[i], grecv.at[there[0], there[1], n or 0], to[via])

    def g_copies(core):
        found, i = {}, 0
        for where, (halves, outs) in plan(core).items():
            found[where] = (halves, [])
            for n, via, there in outs:
                found[where][1].append((i, n, via, there))
                i += 1
        return found

    def choose(i, values):
        got = jnp.int32(values[-1])
        for k in range(len(values) - 1):
            got = jnp.where(i == k, values[k], got)
        return got

    def place(p):
        dx, sy = (
            jnp.where(yhi == 0, *(choose(p, [where[n] for where in order]) for order in orders)) for n in range(2)
        )
        return dx, sy, block(dx, choose(sy, dys))

    def c_copy(p, core):
        yh, q = place(p)[2]
        ref = kv.at[:, yh, :, q, core]
        return remote(ref, ref, csend.at[p], crecv.at[p], device(x, y, z, oc))

    def event(p):
        for half in range(2):
            for core in range(2):
                @pl.when((c == core) & (yhi == half))
                def _(core=core, half=half):
                    where = orders[half][p]
                    halves, outs = g_copies(core)[where]
                    if p:
                        for n in (0, 1) if halves else (None,):
                            ref = piece(*where, n, c)
                            remote(ref, ref, gsend.at[0], grecv.at[where[0], where[1], n or 0], to[0]).wait_recv()
                    for out in outs:
                        g_copy(where, *out).start()

    for dz in range(1, NZ):
        for n in range(2):
            z_landed(rem(z + dz, NZ), n)

    def take_queries():
        for tile in range(TILES):
            for k in range(2):
                if tile or k:
                    q_landed(tile, k)
            for h in range(2):
                part = q_in[tile, :, :, h * DH : (h + 1) * DH].reshape(2 * 64, DH)
                qt[tile, :, h * DH : (h + 1) * DH] = part.T

    mx[...] = jnp.full(mx.shape, -jnp.inf, f32)
    tot[...] = jnp.zeros(tot.shape, f32)
    acc[...] = jnp.zeros(acc.shape, f32)

    def last_slab(t):
        side = jnp.where(t < 4, yhi, 1 - yhi)
        return side * NZ + zsrc(z, rem(t, 4))

    def segment(n, at, g):
        yh, z0, dz, q0, dq = at
        rows = []
        for i in range(CHUNK // DH * g, CHUNK // DH * (g + 1)):
            rows.append(kv[n, yh, z0 + i * dz, q0 + i * dq].reshape(2 * 64, DH))
        return jnp.concatenate(rows, axis=0)

    def fold(v, op):
        return op(v.reshape(v.shape[0] // 8, 8, v.shape[1]), axis=0)

    def score(t, s, g, slot, masked):
        sc = lax.dot_general(
            segment(0, s, g), qt[t], (((1,), (0,)), ((), ())), preferred_element_type=f32
        )
        if masked:
            yl = jnp.where(t < 4, ylo, 1 - ylo)
            row = rem(lax.broadcasted_iota(jnp.int32, sc.shape, 1), 128) + (yl * 4 + x) * 128
            key = lax.broadcasted_iota(jnp.int32, sc.shape, 0) + g * CHUNK
            sc = jnp.where(key <= row, sc, -jnp.inf)
        s_buf[slot, g * CHUNK : (g + 1) * CHUNK] = sc
        return fold(sc, jnp.max)

    def apply(s, g, slot, top8, l8, pv):
        sc = s_buf[slot, g * CHUNK : (g + 1) * CHUNK].reshape(CHUNK // 8, 8, 2 * DH)
        p = jnp.exp2((sc - top8[None]) * SCALE)
        l8 = l8 + jnp.sum(p, axis=0)
        d = lax.dot_general(
            segment(1, s, g), p.reshape(CHUNK, 2 * DH).astype(bf16), (((0,), (0,)), ((), ())),
            preferred_element_type=f32,
        )
        return l8, (d if pv is None else pv + d)

    parts = SLAB // CHUNK

    def o_cols(t):
        return pl.ds(pl.multiple_of((kind * GROUP + 4 * yhi + 2 * c) * DH, 2 * DH), 2 * DH)

    def o_copy(t, k):
        cc = k
        yy = jnp.where(t < 4, y, oy)
        zz = zsrc(z, rem(t, 4))
        return remote(
            o_stage.at[t, cc], o_ref.at[:, o_cols(t)], osend.at[t, cc],
            orecv.at[t, c], device(x, yy, zz, cc),
        )

    def finish(t):
        for h in range(2):
            cols = slice(h * DH, (h + 1) * DH)
            whole = jnp.sum(tot[t, :, cols], axis=0, keepdims=True)
            rows = (acc[t, :, cols] / whole).T.astype(bf16)
            o_stage[t, :, :, cols] = rows.reshape(2, 64, DH)

        for k in range(2):
            @pl.when((t != 0) | (c != k))
            def _():
                o_copy(t, k).start()

    def prep(t, m8):
        old = mx[t]
        top = jnp.maximum(old, jnp.max(m8, axis=0, keepdims=True))
        factor = jnp.exp2((old - top) * SCALE)
        mx[t] = top
        return jnp.broadcast_to(top, (8, 2 * DH)), factor

    def item(t, s, tn, sn, m8, u, masked):
        top8, factor = prep(t, m8)
        l8, pv, nm = tot[t] * factor, None, None
        for g in range(parts):
            r = score(tn, sn, g, 1 - u, masked)
            nm = r if nm is None else jnp.maximum(nm, r)
            l8, pv = apply(s, g, u, top8, l8, pv)
        acc[t] = acc[t] * factor + pv
        tot[t] = l8
        return nm

    near = [zsrc(z, i) for i in range(4)]

    start = yhi
    late = 4 * (1 - yhi)

    def first(t, at, masked):
        m8 = None
        for g in range(parts):
            v = score(t, at, g, 0, masked)
            m8 = v if m8 is None else jnp.maximum(m8, v)
        return m8

    def relay(lo, hi):
        def step(p, _):
            lax.switch(p, [functools.partial(event, i) for i in range(BLOCKS)])
            c_copy(p, c).start()
            return 0

        lax.fori_loop(lo, hi, step, 0)

    def others(lo, hi):
        lax.fori_loop(lo, hi, lambda p, _: (c_copy(p, oc).wait_recv(), 0)[1], 0)

    relay(0, 4)
    take_queries()
    others(0, 4)

    whole = 9 + 3 * yhi

    def about(p):
        _, sy, (_, q) = place(p)
        early = jnp.where(yhi == 0, sy < 2, sy >= 2)
        nc = jnp.where((p < 16) & early, 4, 0)
        second = p >= 16
        slabs = second | ((p >= whole) & (p < whole + 4))
        ts = jnp.where(second, late + 19 - p, jnp.where(slabs, 4 - late + p - whole, 0))
        return p, nc, q, ts, nc + jnp.where(slabs, choose(rem(ts, 4), near) + 1, 0)

    def after(p):
        skip = jnp.where(
            yhi == 0,
            jnp.where(p == 6, 2, jnp.where(p == 12, 4, 1)),
            jnp.where(p == 1, 3, jnp.where((p == 5) | (p == 7), 2, 1)),
        )
        return p + skip

    def what(k, stage):
        p, nc, q, ts, n = stage
        crosses = k < nc
        t = jnp.where(crosses, late + k, ts)
        side = jnp.where(ts < 4, yhi, 1 - yhi)
        dz = jnp.where(crosses, 1, 0)
        at = (
            jnp.where(crosses, 0, side), jnp.where(crosses, 0, k - nc), dz, jnp.where(crosses, q, 0), 1 - dz,
        )
        return t, at, (k + 1 == n) & (n != nc)

    zero = jnp.int32(0)
    stage0 = about(start)
    t0, at0, _ = what(zero, stage0)
    m8 = first(t0, at0, False)
    total = 40 + 2 * (near[0] + near[1] + near[2] + near[3])

    def advance(i, stage, ran, had):
        p = stage[0]
        pn = lax.min(after(p), 19)
        due = lax.max(ran, lax.min(lax.max(FIRST + div(i, PACE), pn + 1), BLOCKS))
        relay(ran, due)
        seen = lax.max(had, lax.min(pn + 1, BLOCKS))
        others(had, seen)
        return about(pn), due, seen

    def pair(i, carry):
        k, stage, ran, had, t, at, m8 = carry
        for h in range(2):
            last = k + 1 == stage[4]
            more, ran, had = lax.cond(
                last,
                lambda stage=stage, ran=ran, had=had: advance(i, stage, ran, had),
                lambda stage=stage, ran=ran, had=had: (stage, ran, had),
            )
            kn = jnp.where(last, 0, k + 1)
            tn, an, diag = what(kn, more)
            m8 = lax.cond(
                diag,
                lambda m8=m8, h=h, a=(t, at, tn, an): item(*a, m8, h, True),
                lambda m8=m8, h=h, a=(t, at, tn, an): item(*a, m8, h, False),
            )

            @pl.when(last & (stage[4] > stage[1]))
            def _(stage=stage):
                finish(stage[3])

            k, stage, t, at = kn, more, tn, an
        return k, stage, ran, had, t, at, m8

    lax.fori_loop(0, div(total, 2), pair, (zero, stage0, zero + 4, zero + 4, t0, at0, m8))
    o_ref[:, o_cols(0)] = o_stage[0, c]

    for tile in range(TILES):
        for k in range(2):
            @pl.when((tile != 0) | (c != k))
            def _(tile=tile, k=k):
                o_copy(jnp.int32(tile), k).wait_send()

    for j in range(4):
        for yy in range(2):
            for k in range(2):
                if j or yy or k:
                    tile = yy * 4 + ZI_OF[j]
                    first_head = rem(tz[j], KV) * GROUP + 4 * div(ys[yy], 2) + 2 * cs[k]
                    cols = pl.ds(pl.multiple_of(first_head * DH, 2 * DH), 2 * DH)
                    remote(
                        o_stage.at[tile, c], o_ref.at[:, cols], osend.at[tile, c], orecv.at[tile, cs[k]],
                        device(x, ys[yy], tz[j], cs[k]),
                    ).wait_recv()

    for core in range(2):
        @pl.when(c == core)
        def _(core=core):
            for where, (_, outs) in g_copies(core).items():
                for out in outs:
                    g_copy(where, *out).wait_send()

    lax.fori_loop(0, BLOCKS, lambda p, _: (c_copy(p, c).wait_send(), 0)[1], 0)
    for dz in z_order:
        for n in range(2):
            z_copy(dz, n).wait_send()
    for yy in (1, 0):
        for j in range(4):
            for k in range(2):
                if j or yy or k:
                    q_copy(j, yy, k).wait_send()


def per_device(queries, keys, values):
    hbm = pl.BlockSpec(memory_space=pl.ANY)
    dma = pltpu.SemaphoreType.DMA
    return pl.pallas_call(
        kernel,
        out_shape=pltpu.VMEM(queries.shape, queries.dtype),
        in_specs=[hbm] * 3,
        out_specs=pl.BlockSpec(memory_space=pltpu.VMEM),
        scratch_shapes=[
            pltpu.VMEM((2, 2, NZ, 8, 2, 64, DH), bf16),
            pltpu.VMEM(queries.shape, bf16),
            pltpu.VMEM(keys.shape, bf16),
            pltpu.VMEM(values.shape, bf16),
            pltpu.VMEM((TILES, 2, 64, 2 * DH), bf16),
            pltpu.VMEM((TILES, DH, 2 * DH), bf16),
            pltpu.VMEM((TILES, 2, 64, 2 * DH), bf16),
            pltpu.VMEM((TILES, 1, 2 * DH), f32),
            pltpu.VMEM((TILES, 8, 2 * DH), f32),
            pltpu.VMEM((TILES, DH, 2 * DH), f32),
            pltpu.VMEM((2, SLAB, 2 * DH), f32),
            dma((5,)),
            dma((2, NZ)), dma((2, NZ)),
            dma((16,)), dma((TILES, 2)),
            dma((24,)), dma((4, 4, 2)),
            dma((16,)), dma((16,)),
            dma((TILES, 2)), dma((TILES, 2)),
        ],
        compiler_params=pltpu.CompilerParams(
            collective_id=0, has_side_effects=True, vmem_limit_bytes=60 * 1024 * 1024
        ),
        name="regrouped_attention",
    )(queries, keys, values)


def solution(mesh):
    spec = P(("seq", "head"), None)
    return jax.shard_map(
        per_device, mesh=mesh, in_specs=(spec, spec, spec), out_specs=spec, check_vma=False
    )
```

```python
import functools
import math

import jax
import jax.numpy as jnp
from jax import lax
from jax.experimental import pallas as pl
from jax.experimental.pallas import tpu as pltpu
from jax.sharding import PartitionSpec as P

H = 32
KV = 4
DH = 128
GROUP = H // KV
NX, NY, NZ = 4, 4, 8
TILES = 8
SLAB = 1024
CHUNK = 512
BLOCKS = NX * NY
PACE = 1
FIRST = 5
SCALE = math.log2(math.e) / math.sqrt(DH)
ZI_OF = (0, 2, 1, 3)
f32 = jnp.float32
bf16 = jnp.bfloat16


def rem(a, b):
    return lax.rem(a, jnp.int32(b))


def div(a, b):
    return lax.div(a, jnp.int32(b))


def tie(z):
    return rem(z + 6 + 4 * rem(div(z, 2), 2), NZ)


def zsrc(z, zi):
    far = rem(z + 6 + 4 * rem(div(z, 2), 2), NZ)
    near = jnp.where(zi == 0, z, jnp.where(zi == 1, rem(z + 1, NZ), rem(z + 7, NZ)))
    return jnp.where(zi == 3, far, near)


def device(x, y, z, c):
    return (div(y, 2) * NZ + z, rem(y, 2) * 8 + x * 2 + c)


def kernel(
    q_hbm, k_hbm, v_hbm, o_ref, kv, q_own, k_own, v_own, q_in, qt, o_stage, mx, tot, acc, s_buf,
    lsem, zsend, zrecv, qsend, qrecv, gsend, grecv, csend, crecv, osend, orecv,
):
    seq = lax.axis_index("seq")
    head = lax.axis_index("head")
    yhi = div(seq, NZ)
    z = rem(seq, NZ)
    ylo = div(head, 8)
    x = rem(div(head, 2), 4)
    c = rem(head, 2)
    y = yhi * 2 + ylo
    oc = 1 - c
    oy = 3 - y
    blk = ylo * 4 + x
    kind = rem(z, KV)

    def remote(src, dst, ssem, rsem, where):
        return pltpu.make_async_remote_copy(
            src_ref=src, dst_ref=dst, send_sem=ssem, recv_sem=rsem,
            device_id=where, device_id_type=pl.DeviceIdType.MESH,
        )

    def local(src, dst, sem):
        return pltpu.make_async_copy(src, dst, sem)

    loads = [
        local(k_hbm, k_own, lsem.at[0]), local(v_hbm, v_own, lsem.at[1]), local(q_hbm, q_own, lsem.at[2]),
    ]
    for load in loads:
        load.start()

    def kv_cols(zz):
        return pl.ds(pl.multiple_of(rem(zz, KV) * DH, DH), DH)

    kept = [
        local(k_hbm.at[:, kv_cols(z)], kv.at[0, yhi, z, blk, c], lsem.at[3]),
        local(v_hbm.at[:, kv_cols(z)], kv.at[1, yhi, z, blk, c], lsem.at[4]),
    ]
    for load in kept:
        load.start()

    tz = [z, rem(z + 1, NZ), rem(z + 7, NZ), tie(z)]
    cs = (c, oc)
    ys = (y, oy)

    barrier = pltpu.get_barrier_semaphore()

    def greet(where):
        pl.semaphore_signal(barrier, inc=1, device_id=where, device_id_type=pl.DeviceIdType.MESH)

    greeted = 0
    for j in range(4):
        for yy in range(2):
            for k in range(2):
                if j or yy or k:
                    greet(device(x, ys[yy], tz[j], cs[k]))
                    greeted += 1
    for zz in (rem(z + 3, NZ), rem(z + 4, NZ), rem(z + 5, NZ), rem(2 * z + NZ - tz[3], NZ)):
        greet(device(x, y, zz, c))
        greeted += 1
    for where in (
        device(rem(x + 1, NX), y, z, c), device(rem(x + 3, NX), y, z, c), device(x, yhi * 2 + 1 - ylo, z, c),
    ):
        greet(where)
        greeted += 1

    mx[...] = jnp.full(mx.shape, -jnp.inf, f32)
    tot[...] = jnp.zeros(tot.shape, f32)
    acc[...] = jnp.zeros(acc.shape, f32)

    for load in loads:
        load.wait()
    pl.semaphore_wait(barrier, greeted)

    own = (k_own, v_own)

    def z_copy(dz, n):
        zz = rem(z + dz, NZ)
        return remote(
            own[n].at[:, kv_cols(zz)], kv.at[n, yhi, z, blk, c], zsend.at[n, dz], zrecv.at[n, z], device(x, y, zz, c)
        )

    def z_landed(zz, n):
        remote(
            own[n].at[:, kv_cols(z)], kv.at[n, yhi, zz, blk, c], zsend.at[n, 0], zrecv.at[n, zz], device(x, y, zz, c)
        ).wait_recv()

    z_order = (4, 3, 5, 2, 6, 1, 7)

    def z_start():
        for dz in z_order:
            for n in range(2):
                z_copy(dz, n).start()

    for load in kept:
        load.wait()

    def q_cols(j, yy, k):
        yh = div(ys[yy], 2)
        first = rem(tz[j], KV) * GROUP + 4 * yh + 2 * cs[k]
        return pl.ds(pl.multiple_of(first * DH, 2 * DH), 2 * DH)

    def q_copy(j, yy, k):
        tile = yy * 4 + ZI_OF[j]
        return remote(
            q_own.at[:, q_cols(j, yy, k)], q_in.at[tile, c], qsend.at[(j * 2 + yy) * 2 + k], qrecv.at[tile, c],
            device(x, ys[yy], tz[j], cs[k]),
        )

    def q_landed(tile, k):
        yy, zi = divmod(tile, 4)
        zz = (z, tz[1], tz[2], tz[3])[zi]
        remote(
            q_own.at[:, pl.ds(0, 2 * DH)], q_in.at[tile, cs[k]], qsend.at[0], qrecv.at[tile, cs[k]],
            device(x, ys[yy], zz, cs[k]),
        ).wait_recv()

    def q_start():
        for yy in (1, 0):
            for j in (3, 1, 2, 0):
                for k in range(2):
                    if j or yy or k:
                        q_copy(j, yy, k).start()

    z_start()
    q_start()

    q_in[0, c] = q_own[:, q_cols(0, 0, 0)]

    din = 1 + 2 * rem(y, 2)
    dys = (0, din, NY - din, 2)
    IN, OUT, FAR = 1, 2, 3
    XUP, XDOWN, YIN, YOUT = range(4)
    to = (
        device(rem(x + 1, NX), y, z, c), device(rem(x + 3, NX), y, z, c),
        device(x, rem(y + dys[IN], NY), z, c), device(x, rem(y + dys[OUT], NY), z, c),
    )
    orders = (
        (
            (0, 0), (3, 0), (1, 0), (0, IN), (2, 0), (3, IN), (1, IN), (0, OUT),
            (2, IN), (3, OUT), (1, OUT), (2, OUT), (0, FAR), (3, FAR), (1, FAR), (2, FAR),
        ),
        (
            (0, 0), (0, OUT), (3, 0), (1, 0), (3, OUT), (1, OUT), (0, IN), (0, FAR),
            (2, 0), (2, OUT), (3, FAR), (1, FAR), (2, FAR), (3, IN), (1, IN), (2, IN),
        ),
    )

    def block(dx, dy):
        xk = rem(x + dx, NX)
        yk = rem(y + dy, NY)
        return div(yk, 2), rem(yk, 2) * 4 + xk

    def piece(dx, sy, n, core):
        yh, q = block(dx, dys[sy])
        if n is None:
            return kv.at[:, yh, :, q, core]
        return kv.at[n, yh, :, q, core]

    def plan(core):
        made = {}
        for dx, sy in orders[0]:
            outs = []
            if (dx, sy) == (0, 0):
                outs += [(None, XUP, (3, 0)), (None, XDOWN, (1, 0)), (None, YIN, (0, IN)), (None, YOUT, (0, OUT))]
            if dx in (3, 1) and (core == 1 or sy == 0):
                outs.append((0, XUP, (2, sy)) if dx == 3 else (1, XDOWN, (2, sy)))
            if core == 0 and sy == 0 and dx:
                outs += [(None, YIN, (dx, IN)), (None, YOUT, (dx, OUT))]
            if core == 1 and dx == 0 and sy:
                outs += [(None, XUP, (3, sy)), (None, XDOWN, (1, sy))]
            if (core == 0 or dx == 0) and sy in (IN, OUT):
                outs.append((0, YOUT, (dx, FAR)) if sy == IN else (1, YIN, (dx, FAR)))
            if core == 0:
                halves = sy == FAR or (dx, sy) == (2, 0)
            else:
                halves = dx == 2 or (dx, sy) == (0, FAR)
            made[dx, sy] = (halves, outs)
        return made

    def g_copy(where, i, n, via, there):
        ref = piece(*where, n, c)
        return remote(ref, ref, gsend.at[i], grecv.at[there[0], there[1], n or 0], to[via])

    def g_copies(core):
        found, i = {}, 0
        for where, (halves, outs) in plan(core).items():
            found[where] = (halves, [])
            for n, via, there in outs:
                found[where][1].append((i, n, via, there))
                i += 1
        return found

    def choose(i, values):
        got = jnp.int32(values[-1])
        for k in range(len(values) - 1):
            got = jnp.where(i == k, values[k], got)
        return got

    def place(p):
        dx, sy = (
            jnp.where(yhi == 0, *(choose(p, [where[n] for where in order]) for order in orders)) for n in range(2)
        )
        return dx, sy, block(dx, choose(sy, dys))

    def c_copy(p, core):
        yh, q = place(p)[2]
        ref = kv.at[:, yh, :, q, core]
        return remote(ref, ref, csend.at[p], crecv.at[p], device(x, y, z, oc))

    def event(p):
        for half in range(2):
            for core in range(2):
                @pl.when((c == core) & (yhi == half))
                def _(core=core, half=half):
                    where = orders[half][p]
                    halves, outs = g_copies(core)[where]
                    if p:
                        for n in (0, 1) if halves else (None,):
                            ref = piece(*where, n, c)
                            remote(ref, ref, gsend.at[0], grecv.at[where[0], where[1], n or 0], to[0]).wait_recv()
                    for out in outs:
                        g_copy(where, *out).start()

    for dz in range(1, NZ):
        for n in range(2):
            z_landed(rem(z + dz, NZ), n)

    def take_queries():
        for tile in range(TILES):
            for k in range(2):
                if tile or k:
                    q_landed(tile, k)
            for h in range(2):
                part = q_in[tile, :, :, h * DH : (h + 1) * DH].reshape(2 * 64, DH)
                qt[tile, :, h * DH : (h + 1) * DH] = part.T


    def last_slab(t):
        side = jnp.where(t < 4, yhi, 1 - yhi)
        return side * NZ + zsrc(z, rem(t, 4))

    def segment(n, at, g):
        yh, z0, dz, q0, dq = at
        rows = []
        for i in range(CHUNK // DH * g, CHUNK // DH * (g + 1)):
            rows.append(kv[n, yh, z0 + i * dz, q0 + i * dq].reshape(2 * 64, DH))
        return jnp.concatenate(rows, axis=0)

    def fold(v, op):
        return op(v.reshape(v.shape[0] // 8, 8, v.shape[1]), axis=0)

    def score(t, s, g, slot, masked):
        sc = lax.dot_general(
            segment(0, s, g), qt[t], (((1,), (0,)), ((), ())), preferred_element_type=f32
        )
        if masked:
            yl = jnp.where(t < 4, ylo, 1 - ylo)
            row = rem(lax.broadcasted_iota(jnp.int32, sc.shape, 1), 128) + (yl * 4 + x) * 128
            key = lax.broadcasted_iota(jnp.int32, sc.shape, 0) + g * CHUNK
            sc = jnp.where(key <= row, sc, -jnp.inf)
        s_buf[slot, g * CHUNK : (g + 1) * CHUNK] = sc
        return fold(sc, jnp.max)

    def apply(s, g, slot, top8, l8, pv):
        sc = s_buf[slot, g * CHUNK : (g + 1) * CHUNK].reshape(CHUNK // 8, 8, 2 * DH)
        p = jnp.exp2((sc - top8[None]) * SCALE)
        l8 = l8 + jnp.sum(p, axis=0)
        d = lax.dot_general(
            segment(1, s, g), p.reshape(CHUNK, 2 * DH).astype(bf16), (((0,), (0,)), ((), ())),
            preferred_element_type=f32,
        )
        return l8, (d if pv is None else pv + d)

    parts = SLAB // CHUNK

    def o_cols(t):
        return pl.ds(pl.multiple_of((kind * GROUP + 4 * yhi + 2 * c) * DH, 2 * DH), 2 * DH)

    def o_copy(t, k):
        cc = k
        yy = jnp.where(t < 4, y, oy)
        zz = zsrc(z, rem(t, 4))
        return remote(
            o_stage.at[t, cc], o_ref.at[:, o_cols(t)], osend.at[t, cc],
            orecv.at[t, c], device(x, yy, zz, cc),
        )

    def finish(t):
        for h in range(2):
            cols = slice(h * DH, (h + 1) * DH)
            whole = jnp.sum(tot[t, :, cols], axis=0, keepdims=True)
            rows = (acc[t, :, cols] / whole).T.astype(bf16)
            o_stage[t, :, :, cols] = rows.reshape(2, 64, DH)

        for k in range(2):
            @pl.when((t != 0) | (c != k))
            def _():
                o_copy(t, k).start()

    def prep(t, m8):
        old = mx[t]
        top = jnp.maximum(old, jnp.max(m8, axis=0, keepdims=True))
        factor = jnp.exp2((old - top) * SCALE)
        mx[t] = top
        return jnp.broadcast_to(top, (8, 2 * DH)), factor

    def item(t, s, tn, sn, m8, u, masked):
        top8, factor = prep(t, m8)
        l8, pv, nm = tot[t] * factor, None, None
        for g in range(parts):
            r = score(tn, sn, g, 1 - u, masked)
            nm = r if nm is None else jnp.maximum(nm, r)
            l8, pv = apply(s, g, u, top8, l8, pv)
        acc[t] = acc[t] * factor + pv
        tot[t] = l8
        return nm

    near = [zsrc(z, i) for i in range(4)]

    start = yhi
    late = 4 * (1 - yhi)

    def first(t, at, masked):
        m8 = None
        for g in range(parts):
            v = score(t, at, g, 0, masked)
            m8 = v if m8 is None else jnp.maximum(m8, v)
        return m8

    def relay(lo, hi):
        def step(p, _):
            lax.switch(p, [functools.partial(event, i) for i in range(BLOCKS)])
            c_copy(p, c).start()
            return 0

        lax.fori_loop(lo, hi, step, 0)

    def others(lo, hi):
        lax.fori_loop(lo, hi, lambda p, _: (c_copy(p, oc).wait_recv(), 0)[1], 0)

    relay(0, 4)
    take_queries()
    others(0, 4)

    whole = 9 + 3 * yhi

    def about(p):
        _, sy, (_, q) = place(p)
        early = jnp.where(yhi == 0, sy < 2, sy >= 2)
        nc = jnp.where((p < 16) & early, 4, 0)
        second = p >= 16
        slabs = second | ((p >= whole) & (p < whole + 4))
        ts = jnp.where(second, late + 19 - p, jnp.where(slabs, 4 - late + p - whole, 0))
        return p, nc, q, ts, nc + jnp.where(slabs, choose(rem(ts, 4), near) + 1, 0)

    def after(p):
        skip = jnp.where(
            yhi == 0,
            jnp.where(p == 6, 2, jnp.where(p == 12, 4, 1)),
            jnp.where(p == 1, 3, jnp.where((p == 5) | (p == 7), 2, 1)),
        )
        return p + skip

    def what(k, stage):
        p, nc, q, ts, n = stage
        crosses = k < nc
        t = jnp.where(crosses, late + k, ts)
        side = jnp.where(ts < 4, yhi, 1 - yhi)
        dz = jnp.where(crosses, 1, 0)
        at = (
            jnp.where(crosses, 0, side), jnp.where(crosses, 0, k - nc), dz, jnp.where(crosses, q, 0), 1 - dz,
        )
        return t, at, (k + 1 == n) & (n != nc)

    zero = jnp.int32(0)
    stage0 = about(start)
    t0, at0, _ = what(zero, stage0)
    m8 = first(t0, at0, False)
    total = 40 + 2 * (near[0] + near[1] + near[2] + near[3])

    def advance(i, stage, ran, had):
        p = stage[0]
        pn = lax.min(after(p), 19)
        due = lax.max(ran, lax.min(lax.max(FIRST + div(i, PACE), pn + 1), BLOCKS))
        relay(ran, due)
        seen = lax.max(had, lax.min(pn + 1, BLOCKS))
        others(had, seen)
        return about(pn), due, seen

    def pair(i, carry):
        k, stage, ran, had, t, at, m8 = carry
        for h in range(2):
            last = k + 1 == stage[4]
            more, ran, had = lax.cond(
                last,
                lambda stage=stage, ran=ran, had=had: advance(i, stage, ran, had),
                lambda stage=stage, ran=ran, had=had: (stage, ran, had),
            )
            kn = jnp.where(last, 0, k + 1)
            tn, an, diag = what(kn, more)
            m8 = lax.cond(
                diag,
                lambda m8=m8, h=h, a=(t, at, tn, an): item(*a, m8, h, True),
                lambda m8=m8, h=h, a=(t, at, tn, an): item(*a, m8, h, False),
            )

            @pl.when(last & (stage[4] > stage[1]))
            def _(stage=stage):
                finish(stage[3])

            k, stage, t, at = kn, more, tn, an
        return k, stage, ran, had, t, at, m8

    lax.fori_loop(0, div(total, 2), pair, (zero, stage0, zero + 4, zero + 4, t0, at0, m8))
    o_ref[:, o_cols(0)] = o_stage[0, c]

    for tile in range(TILES):
        for k in range(2):
            @pl.when((tile != 0) | (c != k))
            def _(tile=tile, k=k):
                o_copy(jnp.int32(tile), k).wait_send()

    for j in range(4):
        for yy in range(2):
            for k in range(2):
                if j or yy or k:
                    tile = yy * 4 + ZI_OF[j]
                    first_head = rem(tz[j], KV) * GROUP + 4 * div(ys[yy], 2) + 2 * cs[k]
                    cols = pl.ds(pl.multiple_of(first_head * DH, 2 * DH), 2 * DH)
                    remote(
                        o_stage.at[tile, c], o_ref.at[:, cols], osend.at[tile, c], orecv.at[tile, cs[k]],
                        device(x, ys[yy], tz[j], cs[k]),
                    ).wait_recv()

    for core in range(2):
        @pl.when(c == core)
        def _(core=core):
            for where, (_, outs) in g_copies(core).items():
                for out in outs:
                    g_copy(where, *out).wait_send()

    lax.fori_loop(0, BLOCKS, lambda p, _: (c_copy(p, c).wait_send(), 0)[1], 0)
    for dz in z_order:
        for n in range(2):
            z_copy(dz, n).wait_send()
    for yy in (1, 0):
        for j in range(4):
            for k in range(2):
                if j or yy or k:
                    q_copy(j, yy, k).wait_send()


def per_device(queries, keys, values):
    hbm = pl.BlockSpec(memory_space=pl.ANY)
    dma = pltpu.SemaphoreType.DMA
    return pl.pallas_call(
        kernel,
        out_shape=pltpu.VMEM(queries.shape, queries.dtype),
        in_specs=[hbm] * 3,
        out_specs=pl.BlockSpec(memory_space=pltpu.VMEM),
        scratch_shapes=[
            pltpu.VMEM((2, 2, NZ, 8, 2, 64, DH), bf16),
            pltpu.VMEM(queries.shape, bf16),
            pltpu.VMEM(keys.shape, bf16),
            pltpu.VMEM(values.shape, bf16),
            pltpu.VMEM((TILES, 2, 64, 2 * DH), bf16),
            pltpu.VMEM((TILES, DH, 2 * DH), bf16),
            pltpu.VMEM((TILES, 2, 64, 2 * DH), bf16),
            pltpu.VMEM((TILES, 1, 2 * DH), f32),
            pltpu.VMEM((TILES, 8, 2 * DH), f32),
            pltpu.VMEM((TILES, DH, 2 * DH), f32),
            pltpu.VMEM((2, SLAB, 2 * DH), f32),
            dma((5,)),
            dma((2, NZ)), dma((2, NZ)),
            dma((16,)), dma((TILES, 2)),
            dma((24,)), dma((4, 4, 2)),
            dma((16,)), dma((16,)),
            dma((TILES, 2)), dma((TILES, 2)),
        ],
        compiler_params=pltpu.CompilerParams(
            collective_id=0, has_side_effects=True, vmem_limit_bytes=60 * 1024 * 1024
        ),
        name="regrouped_attention",
    )(queries, keys, values)


def solution(mesh):
    spec = P(("seq", "head"), None)
    return jax.shard_map(
        per_device, mesh=mesh, in_specs=(spec, spec, spec), out_specs=spec, check_vma=False
    )
```
